256 devices in a mesh: blk: 128 (over z_lo, y, x, core), rep: 2 (over z_hi).
Axes of the slice: x: 4, y: 4, z: 8 (z_hi: 2, z_lo: 4; z = z_hi * 4 + z_lo), core: 2. Of those that a mesh axis runs over, the one named last changes fastest.
Arguments:
- load_coef: bfloat16 [256, 2049, 256], P('blk', None, 'rep'), parts along dimension 2, may hold values from -0.29882812 to 0.29882812
- legendre: bfloat16 [256, 2049, 1024], P('blk'), may hold values from -0.125 to 0.125
- slab_orders: int32 [256], replicated, may hold values from 0 to 1023, as said below
- cycle_rows: int32 [1024], replicated, may hold values from 0 to 1023, each once
Outputs:
- potential: bfloat16 [1024, 128, 4096], P('blk', 'rep'), parts along dimension 1
- energy: float32 [128], P('rep'), parts along dimension 0
The draws below stay inside these ranges and needn't reach their ends.
There are 2 independent parts, one for each index of `rep`. The reference program is written for one: setup_inputs(seed, part) draws one part's arguments, and reference() takes and returns one part's arrays. A program takes and returns all parts, laid end to end along the dimension named above; an argument that names none is the same for every part. Nothing has to cross between parts.
Inputs may be any that keep to these rules, and one draw needn't show every extreme that they name: `slab_orders`: values are distinct and below (2048) / 2. `cycle_rows`: each cycle appears once.
All inputs are finite; a program needn't handle non-finite values.
Results may differ from the reference program's by a relative error of at most 0.0055.
Values may be sent and summed in bfloat16 or wider, within the bound.
A program may use at most 128 MiB of HBM per device.

```python
import math
import jax
import jax.numpy as jnp
from jax import lax

DEGREE = 2047
NLAT = 1024
NLON = 4096
FIELDS = 64
SLAB = 2049
PAIRS = 256


def draw_slab_orders(key, part):
    return jax.random.permutation(key, (DEGREE + 1) // 2)[:PAIRS].astype(jnp.int32)


def levels(key, dims, shards, smallest, top_value):
    loudness = 1.0
    for axis_at, blocks in shards:
        draws = jax.random.uniform(jax.random.fold_in(jax.random.fold_in(key, 6), axis_at), (blocks,), jnp.float32, smallest / len(shards), top_value / len(shards))
        loudness = loudness * jnp.repeat(jnp.exp(draws), dims[axis_at] // blocks).reshape((-1,) + (1,) * (len(dims) - 1 - axis_at))
    return loudness


def scatter_about(key, dims, scale, limit, pieces=(), kind=jnp.bfloat16):
    values = jax.random.normal(key, dims, jnp.float32) * scale
    if len(pieces) > 0:
        values = levels(key, dims, pieces, -0.22, 0.18) * values
    return jnp.clip(values, min=-limit, max=limit).astype(kind)


def setup_inputs(seed: int = 0, part: int = 0) -> dict:
    streams_of = jax.random.split(jax.random.key(seed), 5)
    part_splits = jax.random.split(jax.random.fold_in(streams_of[4], part), 5)
    load_coef = scatter_about(part_splits[0], (PAIRS, SLAB, 2 * FIELDS), 0.05, 0.29882812, ((0, 128),))
    legendre = scatter_about(streams_of[1], (PAIRS, SLAB, NLAT), SLAB ** -0.5, 0.125, ((0, 128),))
    slab_orders = draw_slab_orders(jax.random.fold_in(streams_of[4], 71), part)
    cycle_rows = jax.random.permutation(streams_of[3], NLAT).astype(jnp.int32)
    return {"load_coef": load_coef, "legendre": legendre, "slab_orders": slab_orders, "cycle_rows": cycle_rows}


def basis_table(orders):
    longitude_ids = jnp.arange(NLON, dtype=jnp.int32)
    phase_ids = (orders[:, None] * longitude_ids[None, :]) % NLON
    angles = phase_ids.astype(jnp.float32) * (2.0 * math.pi / NLON)
    factor = jnp.where(orders == 0, 1.0, 2.0).astype(jnp.float32)[:, None]
    return (factor * jnp.cos(angles)).astype(jnp.bfloat16), (-factor * jnp.sin(angles)).astype(jnp.bfloat16)


def reference(load_coef, legendre, slab_orders, cycle_rows):
    slab_rows = DEGREE + 2
    row_ids = jnp.arange(slab_rows, dtype=jnp.int32)

    def synthesize(pair_args):
        pair_coef, pair_table, low_order = pair_args
        in_lower = (row_ids < slab_rows - 1 - low_order)[:, None]
        nothing = jnp.zeros_like(pair_coef)
        stacked = jnp.concatenate([jnp.where(in_lower, pair_coef, nothing), jnp.where(in_lower, nothing, pair_coef)], axis=1)
        return lax.dot_general(stacked, pair_table, (((0,), (0,)), ((), ())), preferred_element_type=jnp.float32).astype(jnp.bfloat16)

    spectra = lax.map(synthesize, (load_coef, legendre, slab_orders))
    spectra = spectra.reshape(PAIRS, 4, FIELDS, NLAT)
    cos_lower, sin_lower = basis_table(slab_orders.astype(jnp.int32))
    cos_upper, sin_upper = basis_table((DEGREE - slab_orders).astype(jnp.int32))
    basis = jnp.stack([cos_lower, sin_lower, cos_upper, sin_upper], axis=1).reshape(PAIRS * 4, NLON)

    def per_field(field_index):
        rows = spectra[:, :, field_index, :].reshape(PAIRS * 4, NLAT)
        wave = lax.dot_general(rows, basis, (((0,), (0,)), ((), ())), preferred_element_type=jnp.float32)
        energy = jnp.sum(wave * wave) / (NLAT * NLON)
        return wave[cycle_rows].astype(jnp.bfloat16), energy

    potential, energy = lax.map(per_field, jnp.arange(FIELDS, dtype=jnp.int32))
    return jnp.transpose(potential, (1, 0, 2)), energy
```

```python
import functools
import math

import jax
import jax.numpy as jnp
from jax import lax
from jax.experimental import pallas as pl
from jax.experimental.pallas import tpu as pltpu
from jax.sharding import PartitionSpec as P

NLON = 4096
HALF = NLON // 2
LANES = 128
MESH = pl.DeviceIdType.MESH
PLANES = 4
SPOTS = 16
CORES = 2
PER_PLANE = SPOTS * CORES
COLUMN = PLANES * CORES
HOPS = (2, 1, 3, 0)


def even_order(low, degree):
    return jnp.where((low & 1) == 0, low, degree - low)


def exchange_kernel(
    table_hbm, coef_hbm, rows_hbm, orders_hbm,
    held_ref, basis_ref, total_ref,
    table, coef, rows_v, orders_v, masked, chosen, spectra, send, recv, wide, partial, near, far,
    in_sem, table_sem, ready_sem, send_sem, recv_sem, near_send, near_recv, far_send, far_recv,
):
    slab_rows, pairs, lat_count = table_hbm.shape
    blocks = table.shape[0]
    block = table.shape[3]
    packed_rows = slab_rows * pairs
    degree = slab_rows - 2
    streams = coef.shape[2]
    fields = streams // 2
    n = PLANES * PER_PLANE
    per_peer = 2 * (lat_count // n)
    cycles = lat_count // n
    plane_rows = PER_PLANE * per_peer

    me = lax.axis_index("blk")
    plane = me // PER_PLANE
    inside = me % PER_PLANE
    spot = inside // CORES
    core = me % CORES

    coef_copy = pltpu.make_async_copy(coef_hbm, coef, in_sem.at[0])
    rows_copy = pltpu.make_async_copy(rows_hbm, rows_v, in_sem.at[1])
    orders_copy = pltpu.make_async_copy(orders_hbm, orders_v, in_sem.at[2])

    def table_copy(b):
        return pltpu.make_async_copy(table_hbm.at[:, :, pl.ds(pl.multiple_of(b * block, block), block)], table.at[b], table_sem.at[b])

    rows_copy.start()
    orders_copy.start()
    coef_copy.start()
    for b in range(blocks):
        table_copy(b).start()

    def column_peer(j):
        q = lax.rem(plane * CORES + core + j, COLUMN)
        return (q // CORES) * PER_PLANE + spot * CORES + q % CORES

    def spot_peer(j):
        return plane * PER_PLANE + lax.rem(spot + j, SPOTS) * CORES + core

    barrier = pltpu.get_barrier_semaphore()

    @pl.loop(1, COLUMN)
    def _(j):
        pl.semaphore_signal(barrier, inc=1, device_id={"blk": column_peer(j)}, device_id_type=MESH)

    @pl.loop(1, SPOTS)
    def _(j):
        pl.semaphore_signal(barrier, inc=1, device_id={"blk": spot_peer(j)}, device_id_type=MESH)

    rows_copy.wait()
    orders_copy.wait()
    columns = jnp.transpose(jnp.broadcast_to(rows_v[...].astype(jnp.float32)[None], (LANES // 8, 8, LANES)).reshape(LANES, LANES))
    cycle_id = lax.broadcasted_iota(jnp.int32, (LANES, lat_count), 1).astype(jnp.float32)
    for part in range(lat_count // LANES):
        chosen[part * LANES : (part + 1) * LANES, :] = (columns[:, part : part + 1] == cycle_id).astype(jnp.float32).astype(jnp.bfloat16)
    orders_row = orders_v[...]
    slot_id = lax.broadcasted_iota(jnp.int32, orders_row.shape, 1)
    lows = [jnp.sum(jnp.where(slot_id == me * pairs + p, orders_row, 0).astype(jnp.float32), axis=1, keepdims=True).astype(jnp.int32) for p in range(pairs)]

    coef_copy.wait()
    packed = coef[...].reshape(packed_rows, streams)
    padding = jnp.zeros((masked.shape[1] - packed_rows, streams), packed.dtype)
    flipped = jnp.transpose(jnp.concatenate([packed, padding], axis=0).astype(jnp.float32))
    packed_id = lax.broadcasted_iota(jnp.int32, (1, masked.shape[1]), 1)
    row_id = packed_id // pairs
    pair_id = packed_id % pairs
    for p in range(pairs):
        lower = (row_id < slab_rows - 1 - lows[p]).astype(jnp.int32)
        is_even = ((lows[p] & 1) == 0).astype(jnp.int32)
        in_even = (lower == is_even).astype(jnp.int32)
        for eo in range(2):
            keep = jnp.where(pair_id == p, jnp.where(in_even == 1 - eo, 1.0, 0.0), 0.0)
            start = (2 * p + eo) * streams
            masked[start : start + streams, :] = jnp.where(jnp.broadcast_to(keep, flipped.shape) > 0.5, flipped, 0.0).astype(jnp.bfloat16)

    pl.semaphore_wait(barrier, COLUMN - 1 + SPOTS - 1)

    @pl.loop(1, SPOTS)
    def _(j):
        pl.semaphore_signal(ready_sem, inc=1, device_id={"blk": spot_peer(j)}, device_id_type=MESH)

    def spectra_of(p, first):
        rows = slice(p * 2 * streams, (p + 1) * 2 * streams)

        @pl.loop(0, blocks)
        def _(b):
            if first:
                table_copy(b).wait()
            product = jnp.dot(masked[rows, :packed_rows], table[b].reshape(packed_rows, block), preferred_element_type=jnp.float32)
            spectra[rows, pl.ds(pl.multiple_of(b * block, block), block)] = product.astype(jnp.bfloat16)

    def sort_plane(p, target):
        count = PER_PLANE * cycles
        picked = chosen[pl.ds(pl.multiple_of(target * count, count), count), :]
        rows = lax.dot_general(picked, spectra[p * 2 * streams : (p + 1) * 2 * streams, :], (((1,), (1,)), ((), ())), preferred_element_type=jnp.float32)
        parts = [rows[:, eo * streams : (eo + 1) * streams].reshape(PER_PLANE, 1, cycles, streams) for eo in range(2)]
        message = jnp.concatenate(parts, axis=1).reshape(plane_rows, streams)
        send[p, pl.ds(pl.multiple_of(target * plane_rows, plane_rows), plane_rows), :] = message.astype(jnp.bfloat16)
        return jnp.sum(rows * rows, axis=0, keepdims=True)

    def block_rows(q):
        return pl.ds(pl.multiple_of(q * per_peer, per_peer), per_peer)

    def send_plane(p, hop):
        target = lax.rem(plane + hop, PLANES)

        @pl.loop(1 if hop == 0 else 0, PER_PLANE)
        def _(i):
            peer = target * PER_PLANE + lax.rem(spot + i // CORES, SPOTS) * CORES + lax.rem(core + i, CORES)
            pltpu.make_async_remote_copy(
                src_ref=send.at[p, block_rows(peer), :], dst_ref=recv.at[p, block_rows(me), :],
                send_sem=send_sem.at[p], recv_sem=recv_sem.at[p],
                device_id={"blk": peer}, device_id_type=MESH).start()

    def all_blocks(p):
        whole = pl.ds(0, (n - 1) * per_peer)
        return pltpu.make_async_remote_copy(
            src_ref=send.at[p, whole, :], dst_ref=recv.at[p, whole, :], send_sem=send_sem.at[p], recv_sem=recv_sem.at[p],
            device_id={"blk": column_peer(1)}, device_id_type=MESH)

    def keep_own(p):
        recv[p, block_rows(me), :] = send[p, block_rows(me), :]

    lane_id = lax.broadcasted_iota(jnp.int32, (1, streams), 1)

    def weighted(p, squares):
        even = even_order(lows[p], degree)
        out = jnp.zeros((1, streams), jnp.float32)
        for eo in range(2):
            order = even if eo == 0 else degree - even
            weight = jnp.where(order == 0, jnp.where(lane_id < fields, 1.0, 0.0), 2.0)
            out = out + weight * squares[:, eo * streams : (eo + 1) * streams]
        return out

    spectra_of(0, True)
    squares = sort_plane(0, lax.rem(plane + HOPS[0], PLANES))
    pl.semaphore_wait(ready_sem, SPOTS - 1)
    for i, hop in enumerate(HOPS):
        if i + 1 < PLANES:
            squares = squares + sort_plane(0, lax.rem(plane + HOPS[i + 1], PLANES))
        send_plane(0, hop)
    keep_own(0)
    energy = weighted(0, squares)

    for p in range(1, pairs):
        spectra_of(p, False)
        squares = sort_plane(p, plane)
        for hop in HOPS[:-1]:
            squares = squares + sort_plane(p, lax.rem(plane + hop, PLANES))
        keep_own(p)
        energy = energy + weighted(p, squares)
    partial[0] = energy

    def near_copy(j):
        return pltpu.make_async_remote_copy(
            src_ref=partial.at[0], dst_ref=near.at[j], send_sem=near_send.at[j], recv_sem=near_recv.at[j],
            device_id={"blk": column_peer(j)}, device_id_type=MESH)

    def far_copy(j):
        return pltpu.make_async_remote_copy(
            src_ref=partial.at[1], dst_ref=far.at[j], send_sem=far_send.at[j], recv_sem=far_recv.at[j],
            device_id={"blk": spot_peer(j)}, device_id_type=MESH)

    send_plane(1, HOPS[0])

    @pl.loop(1, COLUMN)
    def _(j):
        near_copy(j).start()

    for p in range(1, pairs):
        for hop in HOPS[1 if p == 1 else 0 :]:
            send_plane(p, hop)

    scale = 2.0 * math.pi / NLON
    source = lax.broadcasted_iota(jnp.int32, (n, n * pairs), 0)
    slot = lax.broadcasted_iota(jnp.int32, (n, n * pairs), 1)
    lane = lax.broadcasted_iota(jnp.int32, (n, LANES), 1)
    spread = jnp.broadcast_to(orders_row, (n, n * pairs)).astype(jnp.float32)

    @pl.loop(0, 2 * pairs)
    def _(item):
        p = item % pairs
        eo = item // pairs
        low = jnp.sum(jnp.where(slot == source * pairs + p, spread, 0.0), axis=1, keepdims=True).astype(jnp.int32)
        even = even_order(low, degree)
        order = jnp.where(eo == 0, even, degree - even)
        order = jnp.broadcast_to(order, (n, LANES))
        factor = jnp.where(order == 0, 1.0, 2.0)
        coarse_angle = ((order * (LANES * lane)) & (NLON - 1)).astype(jnp.float32) * scale
        fine_angle = ((order * lane) & (NLON - 1)).astype(jnp.float32) * scale
        cos_coarse, sin_coarse = factor * jnp.cos(coarse_angle), factor * jnp.sin(coarse_angle)
        cos_fine, sin_fine = jnp.cos(fine_angle), jnp.sin(fine_angle)
        first = pl.multiple_of(p * 2 * n, 2 * n)
        second = pl.multiple_of(p * 2 * n + n, n)
        for tile in range(HALF // LANES):
            cc, ss = cos_coarse[:, tile : tile + 1], sin_coarse[:, tile : tile + 1]
            lanes = slice(tile * LANES, (tile + 1) * LANES)
            basis_ref[eo, pl.ds(first, n), lanes] = (cc * cos_fine - ss * sin_fine).astype(jnp.bfloat16)
            basis_ref[eo, pl.ds(second, n), lanes] = (-(ss * cos_fine + cc * sin_fine)).astype(jnp.bfloat16)

    def finish(p):
        all_blocks(p).wait_recv()
        wide[...] = recv[p].astype(jnp.float32)
        for eo in range(2):
            for cycle in range(cycles):
                tile = jnp.transpose(wide[pl.ds(eo * cycles + cycle, n, stride=per_peer), :]).astype(jnp.bfloat16)
                rows = slice(cycle * fields, (cycle + 1) * fields)
                held_ref[eo, rows, p * 2 * n : p * 2 * n + n] = tile[:fields]
                held_ref[eo, rows, p * 2 * n + n : (p + 1) * 2 * n] = tile[fields:]

    finish(0)

    @pl.loop(1, COLUMN)
    def _(j):
        near_copy(j).wait()

    partial[1] = partial[0] + jnp.sum(near[1:], axis=0)

    @pl.loop(1, SPOTS)
    def _(j):
        far_copy(j).start()

    for p in range(1, pairs):
        finish(p)

    @pl.loop(1, SPOTS)
    def _(j):
        far_copy(j).wait()

    total_ref[...] = partial[1] + jnp.sum(far[1:], axis=0)
    for p in range(pairs):
        all_blocks(p).wait_send()


def wave_kernel(scale, held_ref, basis_ref, total_ref, out_hbm, energy_ref, out, out_sem):
    cycles, fields, _ = out.shape
    width = 256
    tiles = HALF // width

    def out_copy(tile, side):
        columns = pl.ds(pl.multiple_of(side * HALF + tile * width, width), width)
        return pltpu.make_async_copy(out.at[:, :, columns], out_hbm.at[:, :, columns], out_sem.at[tile, side])

    @pl.loop(0, tiles)
    def _(tile):
        columns = pl.ds(pl.multiple_of(tile * width, width), width)
        even = jnp.dot(held_ref[0], basis_ref[0, :, columns], preferred_element_type=jnp.float32)
        odd = jnp.dot(held_ref[1], basis_ref[1, :, columns], preferred_element_type=jnp.float32)
        out[:, :, columns] = (even + odd).astype(jnp.bfloat16).reshape(cycles, fields, width)
        mirrored = pl.ds(pl.multiple_of(HALF + tile * width, width), width)
        out[:, :, mirrored] = (even - odd).astype(jnp.bfloat16).reshape(cycles, fields, width)
        for side in range(2):
            out_copy(tile, side).start()

    energy_ref[...] = (total_ref[:, :fields] + total_ref[:, fields:]) * scale

    @pl.loop(0, tiles)
    def _(tile):
        for side in range(2):
            out_copy(tile, side).wait()


def shards(load_coef, legendre, slab_orders, cycle_rows):
    n = lax.axis_size("blk")
    pairs, slab_rows, streams = load_coef.shape
    fields = streams // 2
    lat_count = legendre.shape[2]
    cycles = lat_count // n
    packed_rows = slab_rows * pairs
    padded = -(-packed_rows // LANES) * LANES
    per_peer = 2 * cycles
    table = jnp.transpose(legendre, (1, 0, 2))
    coef = jnp.transpose(load_coef, (1, 0, 2))
    blocks = 4
    block = lat_count // blocks
    anywhere = pl.BlockSpec(memory_space=pltpu.HBM)
    vmem = pl.BlockSpec(memory_space=pltpu.VMEM)
    dma = pltpu.SemaphoreType.DMA
    held, basis, total = pl.pallas_call(
        exchange_kernel,
        out_shape=[
            jax.ShapeDtypeStruct((2, cycles * fields, pairs * 2 * n), jnp.bfloat16),
            jax.ShapeDtypeStruct((2, pairs * 2 * n, HALF), jnp.bfloat16),
            jax.ShapeDtypeStruct((1, streams), jnp.float32),
        ],
        in_specs=[anywhere] * 4,
        out_specs=[vmem] * 3,
        scratch_shapes=[
            pltpu.VMEM((blocks, slab_rows, pairs, block), jnp.bfloat16),
            pltpu.VMEM((slab_rows, pairs, streams), jnp.bfloat16),
            pltpu.VMEM((lat_count // LANES, LANES), jnp.int32),
            pltpu.VMEM((1, n * pairs), jnp.int32),
            pltpu.VMEM((2 * pairs * streams, padded), jnp.bfloat16),
            pltpu.VMEM((lat_count, lat_count), jnp.bfloat16),
            pltpu.VMEM((2 * pairs * streams, lat_count), jnp.bfloat16),
            pltpu.VMEM((pairs, n * per_peer, streams), jnp.bfloat16),
            pltpu.VMEM((pairs, n * per_peer, streams), jnp.bfloat16),
            pltpu.VMEM((n * per_peer, streams), jnp.float32),
            pltpu.VMEM((2, 1, streams), jnp.float32),
            pltpu.VMEM((COLUMN, 1, streams), jnp.float32),
            pltpu.VMEM((SPOTS, 1, streams), jnp.float32),
            dma((3,)),
            dma((blocks,)),
            pltpu.SemaphoreType.REGULAR,
            dma((pairs,)),
            dma((pairs,)),
            dma((COLUMN,)),
            dma((COLUMN,)),
            dma((SPOTS,)),
            dma((SPOTS,)),
        ],
        compiler_params=pltpu.CompilerParams(collective_id=0, has_side_effects=True, vmem_limit_bytes=44 * 2**20),
        name="exchange",
    )(table, coef, cycle_rows.reshape(lat_count // LANES, LANES), slab_orders.reshape(1, n * pairs))
    potential, mean_square = pl.pallas_call(
        functools.partial(wave_kernel, 1.0 / lat_count),
        out_shape=[
            jax.ShapeDtypeStruct((cycles, fields, NLON), jnp.bfloat16),
            jax.ShapeDtypeStruct((1, fields), jnp.float32),
        ],
        in_specs=[vmem] * 3,
        out_specs=[anywhere, vmem],
        scratch_shapes=[
            pltpu.VMEM((cycles, fields, NLON), jnp.bfloat16),
            dma((HALF // 256, 2)),
        ],
        compiler_params=pltpu.CompilerParams(vmem_limit_bytes=24 * 2**20),
        name="wave",
    )(held, basis, total)
    return potential, mean_square.reshape(fields)


def solution(mesh):
    in_specs = (P("blk", None, "rep"), P("blk", None, None), P(), P())
    out_specs = (P("blk", "rep", None), P("rep"))
    return jax.shard_map(shards, mesh=mesh, in_specs=in_specs, out_specs=out_specs, check_vma=False)
```

```python
import functools
import math

import jax
import jax.numpy as jnp
from jax import lax
from jax.experimental import pallas as pl
from jax.experimental.pallas import tpu as pltpu
from jax.sharding import PartitionSpec as P

NLON = 4096
HALF = NLON // 2
LANES = 128
MESH = pl.DeviceIdType.MESH
PLANES = 4
SPOTS = 16
CORES = 2
PER_PLANE = SPOTS * CORES
COLUMN = PLANES * CORES
HOPS = (2, 1, 3, 0)


def even_order(low, degree):
    return jnp.where((low & 1) == 0, low, degree - low)


def exchange_kernel(
    table_hbm, coef_hbm, rows_hbm, orders_hbm,
    sum_ref, held_ref, basis_ref, total_ref,
    table, coef, rows_v, orders_v, masked, extra, chosen, spectra, send, recv, wide, partial, near, far, held_first, basis_first,
    in_sem, table_sem, ready_sem, send_sem, recv_sem, near_send, near_recv, far_send, far_recv,
):
    slab_rows, pairs, lat_count = table_hbm.shape
    blocks = table.shape[0]
    block = table.shape[3]
    deep = masked.shape[1]
    last = slab_rows - 1
    degree = slab_rows - 2
    streams = coef.shape[2]
    fields = streams // 2
    n = PLANES * PER_PLANE
    per_peer = 2 * (lat_count // n)
    cycles = lat_count // n
    plane_rows = PER_PLANE * per_peer

    me = lax.axis_index("blk")
    plane = me // PER_PLANE
    inside = me % PER_PLANE
    spot = inside // CORES
    core = me % CORES

    coef_copy = pltpu.make_async_copy(coef_hbm, coef, in_sem.at[0])
    rows_copy = pltpu.make_async_copy(rows_hbm, rows_v, in_sem.at[1])
    orders_copy = pltpu.make_async_copy(orders_hbm, orders_v, in_sem.at[2])

    def table_copy(b):
        return pltpu.make_async_copy(table_hbm.at[:, :, pl.ds(pl.multiple_of(b * block, block), block)], table.at[b], table_sem.at[b])

    rows_copy.start()
    orders_copy.start()
    coef_copy.start()

    def column_peer(j):
        q = lax.rem(plane * CORES + core + j, COLUMN)
        return (q // CORES) * PER_PLANE + spot * CORES + q % CORES

    def spot_peer(j):
        return plane * PER_PLANE + lax.rem(spot + j, SPOTS) * CORES + core

    barrier = pltpu.get_barrier_semaphore()

    @pl.loop(1, COLUMN)
    def _(j):
        pl.semaphore_signal(barrier, inc=1, device_id={"blk": column_peer(j)}, device_id_type=MESH)

    for b in range(blocks):
        table_copy(b).start()

    @pl.loop(1, SPOTS)
    def _(j):
        pl.semaphore_signal(barrier, inc=1, device_id={"blk": spot_peer(j)}, device_id_type=MESH)

    rows_copy.wait()
    orders_copy.wait()
    columns = jnp.transpose(jnp.broadcast_to(rows_v[...].astype(jnp.float32)[None], (LANES // 8, 8, LANES)).reshape(LANES, LANES))
    cycle_id = lax.broadcasted_iota(jnp.int32, (LANES, lat_count), 1).astype(jnp.float32)
    for part in range(lat_count // LANES):
        chosen[part * LANES : (part + 1) * LANES, :] = (columns[:, part : part + 1] == cycle_id).astype(jnp.float32).astype(jnp.bfloat16)
    orders_row = orders_v[...]
    slot_id = lax.broadcasted_iota(jnp.int32, orders_row.shape, 1)
    lows = [jnp.sum(jnp.where(slot_id == me * pairs + p, orders_row, 0).astype(jnp.float32), axis=1, keepdims=True).astype(jnp.int32) for p in range(pairs)]

    coef_copy.wait()
    flipped = jnp.transpose(coef[:last].reshape(deep, streams))
    tail = coef[last].astype(jnp.float32)
    tail = jnp.transpose(jnp.concatenate([tail, jnp.zeros((8 - pairs, streams), jnp.float32)], axis=0))
    packed_id = lax.broadcasted_iota(jnp.int32, (1, deep), 1)
    row_id = packed_id // pairs
    pair_id = packed_id % pairs

    def mask(p):
        is_even = (lows[p] & 1) == 0
        lower = jnp.where(row_id < last - lows[p], 1, 0)
        in_even = lower == jnp.where(is_even, 1, 0)
        for eo in range(2):
            keep = jnp.where(pair_id == p, jnp.where(in_even, 1.0 - eo, 1.0 * eo), 0.0).astype(jnp.bfloat16)
            start = (2 * p + eo) * streams
            masked[start : start + streams, :] = flipped * jnp.broadcast_to(keep, flipped.shape)
            mine = jnp.where(is_even, 1.0 * eo, 1.0 - eo)
            extra[start : start + streams, :] = jnp.broadcast_to(tail[:, p : p + 1] * mine, (streams, LANES))

    mask(0)
    pl.semaphore_wait(barrier, COLUMN - 1 + SPOTS - 1)

    @pl.loop(1, SPOTS)
    def _(j):
        pl.semaphore_signal(ready_sem, inc=1, device_id={"blk": spot_peer(j)}, device_id_type=MESH)

    def spectra_of(p, first):
        rows = slice(p * 2 * streams, (p + 1) * 2 * streams)

        @pl.loop(0, blocks)
        def _(b):
            if first:
                table_copy(b).wait()
            product = jnp.dot(masked[rows, :], table[b, :last].reshape(deep, block), preferred_element_type=jnp.float32)
            row = table[b, last].astype(jnp.float32)[p : p + 1, :]
            product = product + jnp.concatenate([extra[rows, :]] * (block // LANES), axis=1) * row
            spectra[rows, pl.ds(pl.multiple_of(b * block, block), block)] = product.astype(jnp.bfloat16)

    def sort_plane(p, target):
        count = PER_PLANE * cycles
        picked = chosen[pl.ds(pl.multiple_of(target * count, count), count), :]
        rows = lax.dot_general(picked, spectra[p * 2 * streams : (p + 1) * 2 * streams, :], (((1,), (1,)), ((), ())), preferred_element_type=jnp.float32)
        parts = [rows[:, eo * streams : (eo + 1) * streams].reshape(PER_PLANE, 1, cycles, streams) for eo in range(2)]
        message = jnp.concatenate(parts, axis=1).reshape(plane_rows, streams)
        send[p, pl.ds(pl.multiple_of(target * plane_rows, plane_rows), plane_rows), :] = message.astype(jnp.bfloat16)
        return jnp.sum(rows * rows, axis=0, keepdims=True)

    def block_rows(q):
        return pl.ds(pl.multiple_of(q * per_peer, per_peer), per_peer)

    def send_plane(p, hop):
        target = lax.rem(plane + hop, PLANES)

        @pl.loop(1 if hop == 0 else 0, PER_PLANE)
        def _(i):
            peer = target * PER_PLANE + lax.rem(spot + i // CORES, SPOTS) * CORES + lax.rem(core + i, CORES)
            pltpu.make_async_remote_copy(
                src_ref=send.at[p, block_rows(peer), :], dst_ref=recv.at[p, block_rows(me), :],
                send_sem=send_sem.at[p], recv_sem=recv_sem.at[p],
                device_id={"blk": peer}, device_id_type=MESH).start()

    def all_blocks(p):
        whole = pl.ds(0, (n - 1) * per_peer)
        return pltpu.make_async_remote_copy(
            src_ref=send.at[p, whole, :], dst_ref=recv.at[p, whole, :], send_sem=send_sem.at[p], recv_sem=recv_sem.at[p],
            device_id={"blk": column_peer(1)}, device_id_type=MESH)

    def keep_own(p):
        recv[p, block_rows(me), :] = send[p, block_rows(me), :]

    lane_id = lax.broadcasted_iota(jnp.int32, (1, streams), 1)

    def weighted(p, squares):
        even = even_order(lows[p], degree)
        out = jnp.zeros((1, streams), jnp.float32)
        for eo in range(2):
            order = even if eo == 0 else degree - even
            weight = jnp.where(order == 0, jnp.where(lane_id < fields, 1.0, 0.0), 2.0)
            out = out + weight * squares[:, eo * streams : (eo + 1) * streams]
        return out

    spectra_of(0, True)
    squares = sort_plane(0, lax.rem(plane + HOPS[0], PLANES))
    pl.semaphore_wait(ready_sem, SPOTS - 1)
    send_plane(0, HOPS[0])
    for hop in HOPS[1:]:
        squares = squares + sort_plane(0, lax.rem(plane + hop, PLANES))
        send_plane(0, hop)
    keep_own(0)
    energy = weighted(0, squares)
    mask(1)

    for p in range(1, pairs):
        spectra_of(p, False)
        squares = sort_plane(p, plane)
        for hop in HOPS[:-1]:
            squares = squares + sort_plane(p, lax.rem(plane + hop, PLANES))
        keep_own(p)
        energy = energy + weighted(p, squares)
    partial[0] = energy

    def near_copy(j):
        return pltpu.make_async_remote_copy(
            src_ref=partial.at[0], dst_ref=near.at[j], send_sem=near_send.at[j], recv_sem=near_recv.at[j],
            device_id={"blk": column_peer(j)}, device_id_type=MESH)

    def far_copy(j):
        return pltpu.make_async_remote_copy(
            src_ref=partial.at[1], dst_ref=far.at[j], send_sem=far_send.at[j], recv_sem=far_recv.at[j],
            device_id={"blk": spot_peer(j)}, device_id_type=MESH)

    @pl.loop(1, COLUMN)
    def _(j):
        near_copy(j).start()

    send_plane(1, HOPS[0])
    send_plane(1, HOPS[1])

    scale = 2.0 * math.pi / NLON
    source = lax.broadcasted_iota(jnp.int32, (n, n * pairs), 0)
    slot = lax.broadcasted_iota(jnp.int32, (n, n * pairs), 1)
    lane = lax.broadcasted_iota(jnp.int32, (n, LANES), 1)
    spread = jnp.broadcast_to(orders_row, (n, n * pairs)).astype(jnp.float32)

    def fill_basis(p, out, eo):
        low = jnp.sum(jnp.where(slot == source * pairs + p, spread, 0.0), axis=1, keepdims=True).astype(jnp.int32)
        even = even_order(low, degree)
        order = jnp.where(eo == 0, even, degree - even)
        order = jnp.broadcast_to(order, (n, LANES))
        factor = jnp.where(order == 0, 1.0, 2.0)
        coarse_angle = ((order * (LANES * lane)) & (NLON - 1)).astype(jnp.float32) * scale
        fine_angle = ((order * lane) & (NLON - 1)).astype(jnp.float32) * scale
        cos_coarse, sin_coarse = factor * jnp.cos(coarse_angle), factor * jnp.sin(coarse_angle)
        cos_fine, sin_fine = jnp.cos(fine_angle), jnp.sin(fine_angle)
        for tile in range(HALF // LANES):
            cc, ss = cos_coarse[:, tile : tile + 1], sin_coarse[:, tile : tile + 1]
            lanes = slice(tile * LANES, (tile + 1) * LANES)
            out[eo, :n, lanes] = (cc * cos_fine - ss * sin_fine).astype(jnp.bfloat16)
            out[eo, n:, lanes] = (-(ss * cos_fine + cc * sin_fine)).astype(jnp.bfloat16)

    @pl.loop(0, 2)
    def _(eo):
        fill_basis(0, basis_first, eo)

    @pl.loop(1, COLUMN)
    def _(j):
        near_copy(j).wait()

    partial[1] = partial[0] + jnp.sum(near[1:], axis=0)

    @pl.loop(1, SPOTS)
    def _(j):
        far_copy(j).start()

    send_plane(1, HOPS[2])
    send_plane(1, HOPS[3])

    @pl.loop(0, 2)
    def _(eo):
        fill_basis(1, basis_ref, eo)

    def finish(p, out):
        all_blocks(p).wait_recv()
        wide[...] = recv[p].astype(jnp.float32)
        for eo in range(2):
            for cycle in range(cycles):
                tile = jnp.transpose(wide[pl.ds(eo * cycles + cycle, n, stride=per_peer), :]).astype(jnp.bfloat16)
                rows = slice(cycle * fields, (cycle + 1) * fields)
                out[eo, rows, :n] = tile[:fields]
                out[eo, rows, n:] = tile[fields:]

    finish(0, held_first)

    @pl.loop(0, HALF // block)
    def _(tile):
        lanes = pl.ds(pl.multiple_of(tile * block, block), block)
        for eo in range(2):
            sum_ref[eo, :, lanes] = jnp.dot(held_first[eo], basis_first[eo, :, lanes], preferred_element_type=jnp.float32)

    finish(1, held_ref)

    @pl.loop(1, SPOTS)
    def _(j):
        far_copy(j).wait()

    total_ref[...] = partial[1] + jnp.sum(far[1:], axis=0)
    for p in range(pairs):
        all_blocks(p).wait_send()


def wave_kernel(scale, sum_ref, held_ref, basis_ref, total_ref, out_hbm, energy_ref, out, out_sem):
    cycles, fields, _ = out.shape
    width = 256
    tiles = HALF // width

    def out_copy(tile, side):
        columns = pl.ds(pl.multiple_of(side * HALF + tile * width, width), width)
        return pltpu.make_async_copy(out.at[:, :, columns], out_hbm.at[:, :, columns], out_sem.at[tile, side])

    @pl.loop(0, tiles, unroll=8)
    def _(tile):
        columns = pl.ds(pl.multiple_of(tile * width, width), width)
        even = sum_ref[0, :, columns] + jnp.dot(held_ref[0], basis_ref[0, :, columns], preferred_element_type=jnp.float32)
        odd = sum_ref[1, :, columns] + jnp.dot(held_ref[1], basis_ref[1, :, columns], preferred_element_type=jnp.float32)
        out[:, :, columns] = (even + odd).astype(jnp.bfloat16).reshape(cycles, fields, width)
        mirrored = pl.ds(pl.multiple_of(HALF + tile * width, width), width)
        out[:, :, mirrored] = (even - odd).astype(jnp.bfloat16).reshape(cycles, fields, width)
        for side in range(2):
            out_copy(tile, side).start()

    energy_ref[...] = (total_ref[:, :fields] + total_ref[:, fields:]) * scale

    @pl.loop(0, tiles)
    def _(tile):
        for side in range(2):
            out_copy(tile, side).wait()


def shards(load_coef, legendre, slab_orders, cycle_rows):
    n = lax.axis_size("blk")
    pairs, slab_rows, streams = load_coef.shape
    fields = streams // 2
    lat_count = legendre.shape[2]
    cycles = lat_count // n
    deep = (slab_rows - 1) * pairs
    per_peer = 2 * cycles
    table = jnp.transpose(legendre, (1, 0, 2))
    coef = jnp.transpose(load_coef, (1, 0, 2))
    blocks = 4
    block = lat_count // blocks
    anywhere = pl.BlockSpec(memory_space=pltpu.HBM)
    vmem = pl.BlockSpec(memory_space=pltpu.VMEM)
    dma = pltpu.SemaphoreType.DMA
    first, held, basis, total = pl.pallas_call(
        exchange_kernel,
        out_shape=[
            jax.ShapeDtypeStruct((2, cycles * fields, HALF), jnp.float32),
            jax.ShapeDtypeStruct((2, cycles * fields, 2 * n), jnp.bfloat16),
            jax.ShapeDtypeStruct((2, 2 * n, HALF), jnp.bfloat16),
            jax.ShapeDtypeStruct((1, streams), jnp.float32),
        ],
        in_specs=[anywhere] * 4,
        out_specs=[vmem] * 4,
        scratch_shapes=[
            pltpu.VMEM((blocks, slab_rows, pairs, block), jnp.bfloat16),
            pltpu.VMEM((slab_rows, pairs, streams), jnp.bfloat16),
            pltpu.VMEM((lat_count // LANES, LANES), jnp.int32),
            pltpu.VMEM((1, n * pairs), jnp.int32),
            pltpu.VMEM((2 * pairs * streams, deep), jnp.bfloat16),
            pltpu.VMEM((2 * pairs * streams, LANES), jnp.float32),
            pltpu.VMEM((lat_count, lat_count), jnp.bfloat16),
            pltpu.VMEM((2 * pairs * streams, lat_count), jnp.bfloat16),
            pltpu.VMEM((pairs, n * per_peer, streams), jnp.bfloat16),
            pltpu.VMEM((pairs, n * per_peer, streams), jnp.bfloat16),
            pltpu.VMEM((n * per_peer, streams), jnp.float32),
            pltpu.VMEM((2, 1, streams), jnp.float32),
            pltpu.VMEM((COLUMN, 1, streams), jnp.float32),
            pltpu.VMEM((SPOTS, 1, streams), jnp.float32),
            pltpu.VMEM((2, cycles * fields, 2 * n), jnp.bfloat16),
            pltpu.VMEM((2, 2 * n, HALF), jnp.bfloat16),
            dma((3,)),
            dma((blocks,)),
            pltpu.SemaphoreType.REGULAR,
            dma((pairs,)),
            dma((pairs,)),
            dma((COLUMN,)),
            dma((COLUMN,)),
            dma((SPOTS,)),
            dma((SPOTS,)),
        ],
        compiler_params=pltpu.CompilerParams(collective_id=0, has_side_effects=True, vmem_limit_bytes=36 * 2**20),
        name="exchange",
    )(*[pltpu.with_memory_space_constraint(x, pltpu.HBM) for x in (table, coef, cycle_rows.reshape(lat_count // LANES, LANES), slab_orders.reshape(1, n * pairs))])
    potential, mean_square = pl.pallas_call(
        functools.partial(wave_kernel, 1.0 / lat_count),
        out_shape=[
            jax.ShapeDtypeStruct((cycles, fields, NLON), jnp.bfloat16),
            jax.ShapeDtypeStruct((1, fields), jnp.float32),
        ],
        in_specs=[vmem] * 4,
        out_specs=[anywhere, vmem],
        scratch_shapes=[
            pltpu.VMEM((cycles, fields, NLON), jnp.bfloat16),
            dma((HALF // 256, 2)),
        ],
        compiler_params=pltpu.CompilerParams(vmem_limit_bytes=24 * 2**20),
        name="wave",
    )(first, held, basis, total)
    return potential, mean_square.reshape(fields)


def solution(mesh):
    in_specs = (P("blk", None, "rep"), P("blk", None, None), P(), P())
    out_specs = (P("blk", "rep", None), P("rep"))
    return jax.shard_map(shards, mesh=mesh, in_specs=in_specs, out_specs=out_specs, check_vma=False)
```

```python
import functools
import math

import jax
import jax.numpy as jnp
from jax import lax
from jax.experimental import pallas as pl
from jax.experimental.pallas import tpu as pltpu
from jax.sharding import PartitionSpec as P

NLON = 4096
HALF = NLON // 2
LANES = 128
MESH = pl.DeviceIdType.MESH
PLANES = 4
SPOTS = 16
CORES = 2
PER_PLANE = SPOTS * CORES
COLUMN = PLANES * CORES
HOPS = (2, 1, 3, 0)


def even_order(low, degree):
    return jnp.where((low & 1) == 0, low, degree - low)


def exchange_kernel(
    table_hbm, coef_hbm, rows_hbm, orders_hbm,
    sum_ref, held_ref, basis_ref, total_ref,
    table, table_last, coef, rows_v, orders_v, masked, extra, chosen, spectra, send, recv, wide, partial, near, far, held_first, basis_first,
    in_sem, table_sem, ready_sem, send_sem, recv_sem, near_send, near_recv, far_send, far_recv,
):
    slab_rows, pairs, lat_count = table_hbm.shape
    blocks = table.shape[0]
    block = 2 * LANES
    deep = masked.shape[1]
    last = slab_rows - 1
    degree = slab_rows - 2
    streams = coef.shape[2]
    fields = streams // 2
    n = PLANES * PER_PLANE
    per_peer = 2 * (lat_count // n)
    cycles = lat_count // n
    plane_rows = PER_PLANE * per_peer

    me = lax.axis_index("blk")
    plane = me // PER_PLANE
    inside = me % PER_PLANE
    spot = inside // CORES
    core = me % CORES

    coef_copy = pltpu.make_async_copy(coef_hbm, coef, in_sem.at[0])
    rows_copy = pltpu.make_async_copy(rows_hbm, rows_v, in_sem.at[1])
    orders_copy = pltpu.make_async_copy(orders_hbm, orders_v, in_sem.at[2])

    last_copy = pltpu.make_async_copy(table_hbm.at[pl.ds(last, 1)], table_last, in_sem.at[3])

    def table_copy(b):
        flat = table_hbm.reshape(slab_rows * pairs, lat_count)
        return pltpu.make_async_copy(flat.at[pl.ds(0, deep), pl.ds(pl.multiple_of(b * LANES, LANES), LANES)], table.at[b], table_sem.at[b])

    rows_copy.start()
    orders_copy.start()
    last_copy.start()
    coef_copy.start()

    def column_peer(j):
        q = lax.rem(plane * CORES + core + j, COLUMN)
        return (q // CORES) * PER_PLANE + spot * CORES + q % CORES

    def spot_peer(j):
        return plane * PER_PLANE + lax.rem(spot + j, SPOTS) * CORES + core

    barrier = pltpu.get_barrier_semaphore()

    @pl.loop(1, COLUMN)
    def _(j):
        pl.semaphore_signal(barrier, inc=1, device_id={"blk": column_peer(j)}, device_id_type=MESH)

    for b in range(blocks):
        table_copy(b).start()

    @pl.loop(1, SPOTS)
    def _(j):
        pl.semaphore_signal(barrier, inc=1, device_id={"blk": spot_peer(j)}, device_id_type=MESH)

    rows_copy.wait()
    orders_copy.wait()
    last_copy.wait()
    columns = jnp.transpose(jnp.broadcast_to(rows_v[...].astype(jnp.float32)[None], (LANES // 8, 8, LANES)).reshape(LANES, LANES))
    cycle_id = lax.broadcasted_iota(jnp.int32, (LANES, lat_count), 1).astype(jnp.float32)
    for part in range(lat_count // LANES):
        chosen[part * LANES : (part + 1) * LANES, :] = (columns[:, part : part + 1] == cycle_id).astype(jnp.float32).astype(jnp.bfloat16)
    orders_row = orders_v[...]
    slot_id = lax.broadcasted_iota(jnp.int32, orders_row.shape, 1)
    lows = [jnp.sum(jnp.where(slot_id == me * pairs + p, orders_row, 0).astype(jnp.float32), axis=1, keepdims=True).astype(jnp.int32) for p in range(pairs)]

    coef_copy.wait()
    flipped = jnp.transpose(coef[:last].reshape(deep, streams))
    tail = coef[last].astype(jnp.float32)
    tail = jnp.transpose(jnp.concatenate([tail, jnp.zeros((8 - pairs, streams), jnp.float32)], axis=0))
    packed_id = lax.broadcasted_iota(jnp.int32, (1, deep), 1)
    row_id = packed_id // pairs
    pair_id = packed_id % pairs

    def mask(p):
        is_even = (lows[p] & 1) == 0
        lower = jnp.where(row_id < last - lows[p], 1, 0)
        in_even = lower == jnp.where(is_even, 1, 0)
        for eo in range(2):
            keep = jnp.where(pair_id == p, jnp.where(in_even, 1.0 - eo, 1.0 * eo), 0.0).astype(jnp.bfloat16)
            start = (2 * p + eo) * streams
            masked[start : start + streams, :] = flipped * jnp.broadcast_to(keep, flipped.shape)
            mine = jnp.where(is_even, 1.0 * eo, 1.0 - eo)
            extra[start : start + streams, :] = jnp.broadcast_to(tail[:, p : p + 1] * mine, (streams, LANES))

    mask(0)
    pl.semaphore_wait(barrier, COLUMN - 1 + SPOTS - 1)

    @pl.loop(1, SPOTS)
    def _(j):
        pl.semaphore_signal(ready_sem, inc=1, device_id={"blk": spot_peer(j)}, device_id_type=MESH)

    def spectra_of(p, first):
        rows = slice(p * 2 * streams, (p + 1) * 2 * streams)

        @pl.loop(0, lat_count // block)
        def _(b):
            if first:
                table_copy(2 * b).wait()
                table_copy(2 * b + 1).wait()
            right = jnp.concatenate([table[2 * b + i] for i in range(2)], axis=1)
            product = jnp.dot(masked[rows, :], right, preferred_element_type=jnp.float32)
            row = table_last[0, :, pl.ds(pl.multiple_of(b * block, block), block)].astype(jnp.float32)[p : p + 1, :]
            product = product + jnp.concatenate([extra[rows, :]] * (block // LANES), axis=1) * row
            spectra[rows, pl.ds(pl.multiple_of(b * block, block), block)] = product.astype(jnp.bfloat16)

    def sort_plane(p, target):
        count = PER_PLANE * cycles
        picked = chosen[pl.ds(pl.multiple_of(target * count, count), count), :]
        rows = lax.dot_general(picked, spectra[p * 2 * streams : (p + 1) * 2 * streams, :], (((1,), (1,)), ((), ())), preferred_element_type=jnp.float32)
        parts = [rows[:, eo * streams : (eo + 1) * streams].reshape(PER_PLANE, 1, cycles, streams) for eo in range(2)]
        message = jnp.concatenate(parts, axis=1).reshape(plane_rows, streams)
        send[p, pl.ds(pl.multiple_of(target * plane_rows, plane_rows), plane_rows), :] = message.astype(jnp.bfloat16)
        return jnp.sum(rows * rows, axis=0, keepdims=True)

    def block_rows(q):
        return pl.ds(pl.multiple_of(q * per_peer, per_peer), per_peer)

    def send_plane(p, hop):
        target = lax.rem(plane + hop, PLANES)

        @pl.loop(1 if hop == 0 else 0, PER_PLANE)
        def _(i):
            peer = target * PER_PLANE + lax.rem(spot + i // CORES, SPOTS) * CORES + lax.rem(core + i, CORES)
            pltpu.make_async_remote_copy(
                src_ref=send.at[p, block_rows(peer), :], dst_ref=recv.at[p, block_rows(me), :],
                send_sem=send_sem.at[p], recv_sem=recv_sem.at[p],
                device_id={"blk": peer}, device_id_type=MESH).start()

    def all_blocks(p):
        whole = pl.ds(0, (n - 1) * per_peer)
        return pltpu.make_async_remote_copy(
            src_ref=send.at[p, whole, :], dst_ref=recv.at[p, whole, :], send_sem=send_sem.at[p], recv_sem=recv_sem.at[p],
            device_id={"blk": column_peer(1)}, device_id_type=MESH)

    def keep_own(p):
        recv[p, block_rows(me), :] = send[p, block_rows(me), :]

    lane_id = lax.broadcasted_iota(jnp.int32, (1, streams), 1)

    def weighted(p, squares):
        even = even_order(lows[p], degree)
        out = jnp.zeros((1, streams), jnp.float32)
        for eo in range(2):
            order = even if eo == 0 else degree - even
            weight = jnp.where(order == 0, jnp.where(lane_id < fields, 1.0, 0.0), 2.0)
            out = out + weight * squares[:, eo * streams : (eo + 1) * streams]
        return out

    spectra_of(0, True)
    squares = sort_plane(0, lax.rem(plane + HOPS[0], PLANES))
    pl.semaphore_wait(ready_sem, SPOTS - 1)
    send_plane(0, HOPS[0])
    for hop in HOPS[1:]:
        squares = squares + sort_plane(0, lax.rem(plane + hop, PLANES))
        send_plane(0, hop)
    keep_own(0)
    energy = weighted(0, squares)
    mask(1)

    for p in range(1, pairs):
        spectra_of(p, False)
        squares = sort_plane(p, plane)
        for hop in HOPS[:-1]:
            squares = squares + sort_plane(p, lax.rem(plane + hop, PLANES))
        keep_own(p)
        energy = energy + weighted(p, squares)
    partial[0] = energy

    def near_copy(j):
        return pltpu.make_async_remote_copy(
            src_ref=partial.at[0], dst_ref=near.at[j], send_sem=near_send.at[j], recv_sem=near_recv.at[j],
            device_id={"blk": column_peer(j)}, device_id_type=MESH)

    def far_copy(j):
        return pltpu.make_async_remote_copy(
            src_ref=partial.at[1], dst_ref=far.at[j], send_sem=far_send.at[j], recv_sem=far_recv.at[j],
            device_id={"blk": spot_peer(j)}, device_id_type=MESH)

    @pl.loop(1, COLUMN)
    def _(j):
        near_copy(j).start()

    send_plane(1, HOPS[0])
    send_plane(1, HOPS[1])

    scale = 2.0 * math.pi / NLON
    source = lax.broadcasted_iota(jnp.int32, (n, n * pairs), 0)
    slot = lax.broadcasted_iota(jnp.int32, (n, n * pairs), 1)
    lane = lax.broadcasted_iota(jnp.int32, (n, LANES), 1)
    spread = jnp.broadcast_to(orders_row, (n, n * pairs)).astype(jnp.float32)

    def fill_basis(p, out, eo):
        low = jnp.sum(jnp.where(slot == source * pairs + p, spread, 0.0), axis=1, keepdims=True).astype(jnp.int32)
        even = even_order(low, degree)
        order = jnp.where(eo == 0, even, degree - even)
        order = jnp.broadcast_to(order, (n, LANES))
        factor = jnp.where(order == 0, 1.0, 2.0)
        coarse_angle = ((order * (LANES * lane)) & (NLON - 1)).astype(jnp.float32) * scale
        fine_angle = ((order * lane) & (NLON - 1)).astype(jnp.float32) * scale
        cos_coarse, sin_coarse = factor * jnp.cos(coarse_angle), factor * jnp.sin(coarse_angle)
        cos_fine, sin_fine = jnp.cos(fine_angle), jnp.sin(fine_angle)
        for tile in range(HALF // LANES):
            cc, ss = cos_coarse[:, tile : tile + 1], sin_coarse[:, tile : tile + 1]
            lanes = slice(tile * LANES, (tile + 1) * LANES)
            out[eo, :n, lanes] = (cc * cos_fine - ss * sin_fine).astype(jnp.bfloat16)
            out[eo, n:, lanes] = (-(ss * cos_fine + cc * sin_fine)).astype(jnp.bfloat16)

    @pl.loop(0, 2)
    def _(eo):
        fill_basis(0, basis_first, eo)

    @pl.loop(1, COLUMN)
    def _(j):
        near_copy(j).wait()

    partial[1] = partial[0] + jnp.sum(near[1:], axis=0)

    @pl.loop(1, SPOTS)
    def _(j):
        far_copy(j).start()

    send_plane(1, HOPS[2])
    send_plane(1, HOPS[3])

    @pl.loop(0, 2)
    def _(eo):
        fill_basis(1, basis_ref, eo)

    def finish(p, out):
        all_blocks(p).wait_recv()
        wide[...] = recv[p].astype(jnp.float32)
        for eo in range(2):
            for cycle in range(cycles):
                tile = jnp.transpose(wide[pl.ds(eo * cycles + cycle, n, stride=per_peer), :]).astype(jnp.bfloat16)
                rows = slice(cycle * fields, (cycle + 1) * fields)
                out[eo, rows, :n] = tile[:fields]
                out[eo, rows, n:] = tile[fields:]

    finish(0, held_first)

    @pl.loop(0, HALF // block)
    def _(tile):
        lanes = pl.ds(pl.multiple_of(tile * block, block), block)
        for eo in range(2):
            sum_ref[eo, :, lanes] = jnp.dot(held_first[eo], basis_first[eo, :, lanes], preferred_element_type=jnp.float32)

    finish(1, held_ref)

    @pl.loop(1, SPOTS)
    def _(j):
        far_copy(j).wait()

    total_ref[...] = partial[1] + jnp.sum(far[1:], axis=0)
    for p in range(pairs):
        all_blocks(p).wait_send()


def wave_kernel(scale, sum_ref, held_ref, basis_ref, total_ref, out_hbm, energy_ref, out, out_sem):
    cycles, fields, _ = out.shape
    width = 256
    tiles = HALF // width

    def out_copy(tile, side):
        columns = pl.ds(pl.multiple_of(side * HALF + tile * width, width), width)
        return pltpu.make_async_copy(out.at[:, :, columns], out_hbm.at[:, :, columns], out_sem.at[tile, side])

    @pl.loop(0, tiles, unroll=8)
    def _(tile):
        columns = pl.ds(pl.multiple_of(tile * width, width), width)
        even = sum_ref[0, :, columns] + jnp.dot(held_ref[0], basis_ref[0, :, columns], preferred_element_type=jnp.float32)
        odd = sum_ref[1, :, columns] + jnp.dot(held_ref[1], basis_ref[1, :, columns], preferred_element_type=jnp.float32)
        out[:, :, columns] = (even + odd).astype(jnp.bfloat16).reshape(cycles, fields, width)
        mirrored = pl.ds(pl.multiple_of(HALF + tile * width, width), width)
        out[:, :, mirrored] = (even - odd).astype(jnp.bfloat16).reshape(cycles, fields, width)
        for side in range(2):
            out_copy(tile, side).start()

    energy_ref[...] = (total_ref[:, :fields] + total_ref[:, fields:]) * scale

    @pl.loop(0, tiles)
    def _(tile):
        for side in range(2):
            out_copy(tile, side).wait()


def shards(load_coef, legendre, slab_orders, cycle_rows):
    n = lax.axis_size("blk")
    pairs, slab_rows, streams = load_coef.shape
    fields = streams // 2
    lat_count = legendre.shape[2]
    cycles = lat_count // n
    deep = (slab_rows - 1) * pairs
    per_peer = 2 * cycles
    table = jnp.transpose(legendre, (1, 0, 2))
    coef = jnp.transpose(load_coef, (1, 0, 2))
    blocks = lat_count // LANES
    anywhere = pl.BlockSpec(memory_space=pltpu.HBM)
    vmem = pl.BlockSpec(memory_space=pltpu.VMEM)
    dma = pltpu.SemaphoreType.DMA
    first, held, basis, total = pl.pallas_call(
        exchange_kernel,
        out_shape=[
            jax.ShapeDtypeStruct((2, cycles * fields, HALF), jnp.float32),
            jax.ShapeDtypeStruct((2, cycles * fields, 2 * n), jnp.bfloat16),
            jax.ShapeDtypeStruct((2, 2 * n, HALF), jnp.bfloat16),
            jax.ShapeDtypeStruct((1, streams), jnp.float32),
        ],
        in_specs=[anywhere] * 4,
        out_specs=[vmem] * 4,
        scratch_shapes=[
            pltpu.VMEM((blocks, deep, LANES), jnp.bfloat16),
            pltpu.VMEM((1, pairs, lat_count), jnp.bfloat16),
            pltpu.VMEM((slab_rows, pairs, streams), jnp.bfloat16),
            pltpu.VMEM((lat_count // LANES, LANES), jnp.int32),
            pltpu.VMEM((1, n * pairs), jnp.int32),
            pltpu.VMEM((2 * pairs * streams, deep), jnp.bfloat16),
            pltpu.VMEM((2 * pairs * streams, LANES), jnp.float32),
            pltpu.VMEM((lat_count, lat_count), jnp.bfloat16),
            pltpu.VMEM((2 * pairs * streams, lat_count), jnp.bfloat16),
            pltpu.VMEM((pairs, n * per_peer, streams), jnp.bfloat16),
            pltpu.VMEM((pairs, n * per_peer, streams), jnp.bfloat16),
            pltpu.VMEM((n * per_peer, streams), jnp.float32),
            pltpu.VMEM((2, 1, streams), jnp.float32),
            pltpu.VMEM((COLUMN, 1, streams), jnp.float32),
            pltpu.VMEM((SPOTS, 1, streams), jnp.float32),
            pltpu.VMEM((2, cycles * fields, 2 * n), jnp.bfloat16),
            pltpu.VMEM((2, 2 * n, HALF), jnp.bfloat16),
            dma((4,)),
            dma((blocks,)),
            pltpu.SemaphoreType.REGULAR,
            dma((pairs,)),
            dma((pairs,)),
            dma((COLUMN,)),
            dma((COLUMN,)),
            dma((SPOTS,)),
            dma((SPOTS,)),
        ],
        compiler_params=pltpu.CompilerParams(collective_id=0, has_side_effects=True, vmem_limit_bytes=36 * 2**20),
        name="exchange",
    )(*[pltpu.with_memory_space_constraint(x, pltpu.HBM) for x in (table, coef, cycle_rows.reshape(lat_count // LANES, LANES), slab_orders.reshape(1, n * pairs))])
    potential, mean_square = pl.pallas_call(
        functools.partial(wave_kernel, 1.0 / lat_count),
        out_shape=[
            jax.ShapeDtypeStruct((cycles, fields, NLON), jnp.bfloat16),
            jax.ShapeDtypeStruct((1, fields), jnp.float32),
        ],
        in_specs=[vmem] * 4,
        out_specs=[anywhere, vmem],
        scratch_shapes=[
            pltpu.VMEM((cycles, fields, NLON), jnp.bfloat16),
            dma((HALF // 256, 2)),
        ],
        compiler_params=pltpu.CompilerParams(vmem_limit_bytes=24 * 2**20),
        name="wave",
    )(first, held, basis, total)
    return potential, mean_square.reshape(fields)


def solution(mesh):
    in_specs = (P("blk", None, "rep"), P("blk", None, None), P(), P())
    out_specs = (P("blk", "rep", None), P("rep"))
    return jax.shard_map(shards, mesh=mesh, in_specs=in_specs, out_specs=out_specs, check_vma=False)
```

```python
import functools
import math

import jax
import jax.numpy as jnp
from jax import lax
from jax.experimental import pallas as pl
from jax.experimental.pallas import tpu as pltpu
from jax.sharding import PartitionSpec as P

NLON = 4096
HALF = NLON // 2
LANES = 128
MESH = pl.DeviceIdType.MESH
PLANES = 4
SPOTS = 16
CORES = 2
PER_PLANE = SPOTS * CORES
COLUMN = PLANES * CORES
HOPS = (2, 1, 3, 0)


def even_order(low, degree):
    return jnp.where((low & 1) == 0, low, degree - low)


def exchange_kernel(
    table_hbm, coef_hbm, rows_hbm, orders_hbm,
    sum_ref, held_ref, basis_ref, total_ref,
    table, table_last, coef, coef_last, rows_v, orders_v, masked, extra, chosen, spectra, send, recv, wide, partial, near, far, held_first, basis_first,
    in_sem, table_sem, ready_sem, send_sem, recv_sem, near_send, near_recv, far_send, far_recv,
):
    slab_rows, pairs, lat_count = table_hbm.shape
    blocks = table.shape[0]
    block = 2 * LANES
    deep = masked.shape[1]
    last = slab_rows - 1
    degree = slab_rows - 2
    streams = coef.shape[1]
    fields = streams // 2
    n = PLANES * PER_PLANE
    per_peer = 2 * (lat_count // n)
    cycles = lat_count // n
    plane_rows = PER_PLANE * per_peer

    me = lax.axis_index("blk")
    plane = me // PER_PLANE
    inside = me % PER_PLANE
    spot = inside // CORES
    core = me % CORES

    coef_copy = pltpu.make_async_copy(coef_hbm.reshape(slab_rows * pairs, streams).at[pl.ds(0, deep)], coef, in_sem.at[0])
    tail_copy = pltpu.make_async_copy(coef_hbm.at[pl.ds(last, 1)], coef_last, in_sem.at[4])
    rows_copy = pltpu.make_async_copy(rows_hbm, rows_v, in_sem.at[1])
    orders_copy = pltpu.make_async_copy(orders_hbm, orders_v, in_sem.at[2])

    last_copy = pltpu.make_async_copy(table_hbm.at[pl.ds(last, 1)], table_last, in_sem.at[3])

    def table_copy(b):
        flat = table_hbm.reshape(slab_rows * pairs, lat_count)
        return pltpu.make_async_copy(flat.at[pl.ds(0, deep), pl.ds(pl.multiple_of(b * LANES, LANES), LANES)], table.at[b], table_sem.at[b])

    rows_copy.start()
    orders_copy.start()
    last_copy.start()
    tail_copy.start()
    coef_copy.start()

    def column_peer(j):
        q = lax.rem(plane * CORES + core + j, COLUMN)
        return (q // CORES) * PER_PLANE + spot * CORES + q % CORES

    def spot_peer(j):
        return plane * PER_PLANE + lax.rem(spot + j, SPOTS) * CORES + core

    barrier = pltpu.get_barrier_semaphore()

    @pl.loop(1, COLUMN)
    def _(j):
        pl.semaphore_signal(barrier, inc=1, device_id={"blk": column_peer(j)}, device_id_type=MESH)

    for b in range(blocks):
        table_copy(b).start()

    @pl.loop(1, SPOTS)
    def _(j):
        pl.semaphore_signal(barrier, inc=1, device_id={"blk": spot_peer(j)}, device_id_type=MESH)

    rows_copy.wait()
    orders_copy.wait()
    last_copy.wait()
    tail_copy.wait()
    columns = jnp.transpose(jnp.broadcast_to(rows_v[...].astype(jnp.float32)[None], (LANES // 8, 8, LANES)).reshape(LANES, LANES))
    cycle_id = lax.broadcasted_iota(jnp.int32, (LANES, lat_count), 1).astype(jnp.float32)
    for part in range(lat_count // LANES):
        chosen[part * LANES : (part + 1) * LANES, :] = (columns[:, part : part + 1] == cycle_id).astype(jnp.float32).astype(jnp.bfloat16)
    orders_row = orders_v[...]
    slot_id = lax.broadcasted_iota(jnp.int32, orders_row.shape, 1)
    lows = [jnp.sum(jnp.where(slot_id == me * pairs + p, orders_row, 0).astype(jnp.float32), axis=1, keepdims=True).astype(jnp.int32) for p in range(pairs)]

    coef_copy.wait()
    flipped = jnp.transpose(coef[...])
    tail = coef_last[0].astype(jnp.float32)
    tail = jnp.transpose(jnp.concatenate([tail, jnp.zeros((8 - pairs, streams), jnp.float32)], axis=0))
    packed_id = lax.broadcasted_iota(jnp.int32, (1, deep), 1)
    row_id = packed_id // pairs
    pair_id = packed_id % pairs

    def mask(p):
        is_even = (lows[p] & 1) == 0
        lower = jnp.where(row_id < last - lows[p], 1, 0)
        in_even = lower == jnp.where(is_even, 1, 0)
        for eo in range(2):
            keep = jnp.where(pair_id == p, jnp.where(in_even, 1.0 - eo, 1.0 * eo), 0.0).astype(jnp.bfloat16)
            start = (2 * p + eo) * streams
            masked[start : start + streams, :] = flipped * jnp.broadcast_to(keep, flipped.shape)
            mine = jnp.where(is_even, 1.0 * eo, 1.0 - eo)
            extra[start : start + streams, :] = jnp.broadcast_to(tail[:, p : p + 1] * mine, (streams, LANES))

    mask(0)
    pl.semaphore_wait(barrier, COLUMN - 1 + SPOTS - 1)

    @pl.loop(1, SPOTS)
    def _(j):
        pl.semaphore_signal(ready_sem, inc=1, device_id={"blk": spot_peer(j)}, device_id_type=MESH)

    def spectra_of(p, first):
        rows = slice(p * 2 * streams, (p + 1) * 2 * streams)

        @pl.loop(0, lat_count // block)
        def _(b):
            if first:
                table_copy(2 * b).wait()
                table_copy(2 * b + 1).wait()
            right = jnp.concatenate([table[2 * b + i] for i in range(2)], axis=1)
            product = jnp.dot(masked[rows, :], right, preferred_element_type=jnp.float32)
            row = table_last[0, :, pl.ds(pl.multiple_of(b * block, block), block)].astype(jnp.float32)[p : p + 1, :]
            product = product + jnp.concatenate([extra[rows, :]] * (block // LANES), axis=1) * row
            spectra[rows, pl.ds(pl.multiple_of(b * block, block), block)] = product.astype(jnp.bfloat16)

    def sort_plane(p, target):
        count = PER_PLANE * cycles
        picked = chosen[pl.ds(pl.multiple_of(target * count, count), count), :]
        rows = lax.dot_general(picked, spectra[p * 2 * streams : (p + 1) * 2 * streams, :], (((1,), (1,)), ((), ())), preferred_element_type=jnp.float32)
        parts = [rows[:, eo * streams : (eo + 1) * streams].reshape(PER_PLANE, 1, cycles, streams) for eo in range(2)]
        message = jnp.concatenate(parts, axis=1).reshape(plane_rows, streams)
        send[p, pl.ds(pl.multiple_of(target * plane_rows, plane_rows), plane_rows), :] = message.astype(jnp.bfloat16)
        return jnp.sum(rows * rows, axis=0, keepdims=True)

    def block_rows(q):
        return pl.ds(pl.multiple_of(q * per_peer, per_peer), per_peer)

    def send_plane(p, hop):
        target = lax.rem(plane + hop, PLANES)

        @pl.loop(1 if hop == 0 else 0, PER_PLANE)
        def _(i):
            peer = target * PER_PLANE + lax.rem(spot + i // CORES, SPOTS) * CORES + lax.rem(core + i, CORES)
            pltpu.make_async_remote_copy(
                src_ref=send.at[p, block_rows(peer), :], dst_ref=recv.at[p, block_rows(me), :],
                send_sem=send_sem.at[p], recv_sem=recv_sem.at[p],
                device_id={"blk": peer}, device_id_type=MESH).start()

    def all_blocks(p):
        whole = pl.ds(0, (n - 1) * per_peer)
        return pltpu.make_async_remote_copy(
            src_ref=send.at[p, whole, :], dst_ref=recv.at[p, whole, :], send_sem=send_sem.at[p], recv_sem=recv_sem.at[p],
            device_id={"blk": column_peer(1)}, device_id_type=MESH)

    def keep_own(p):
        recv[p, block_rows(me), :] = send[p, block_rows(me), :]

    lane_id = lax.broadcasted_iota(jnp.int32, (1, streams), 1)

    def weighted(p, squares):
        even = even_order(lows[p], degree)
        out = jnp.zeros((1, streams), jnp.float32)
        for eo in range(2):
            order = even if eo == 0 else degree - even
            weight = jnp.where(order == 0, jnp.where(lane_id < fields, 1.0, 0.0), 2.0)
            out = out + weight * squares[:, eo * streams : (eo + 1) * streams]
        return out

    spectra_of(0, True)
    squares = sort_plane(0, lax.rem(plane + HOPS[0], PLANES))
    pl.semaphore_wait(ready_sem, SPOTS - 1)
    send_plane(0, HOPS[0])
    for hop in HOPS[1:]:
        squares = squares + sort_plane(0, lax.rem(plane + hop, PLANES))
        send_plane(0, hop)
    keep_own(0)
    energy = weighted(0, squares)
    mask(1)

    for p in range(1, pairs):
        spectra_of(p, False)
        squares = sort_plane(p, plane)
        for hop in HOPS[:-1]:
            squares = squares + sort_plane(p, lax.rem(plane + hop, PLANES))
        keep_own(p)
        energy = energy + weighted(p, squares)
    partial[0] = energy

    def near_copy(j):
        return pltpu.make_async_remote_copy(
            src_ref=partial.at[1], dst_ref=near.at[j], send_sem=near_send.at[j], recv_sem=near_recv.at[j],
            device_id={"blk": column_peer(j)}, device_id_type=MESH)

    def far_copy(j):
        return pltpu.make_async_remote_copy(
            src_ref=partial.at[0], dst_ref=far.at[j], send_sem=far_send.at[j], recv_sem=far_recv.at[j],
            device_id={"blk": spot_peer(j)}, device_id_type=MESH)

    @pl.loop(1, SPOTS)
    def _(j):
        far_copy(j).start()

    for hop in HOPS:
        send_plane(1, hop)

    scale = 2.0 * math.pi / NLON
    source = lax.broadcasted_iota(jnp.int32, (n, n * pairs), 0)
    slot = lax.broadcasted_iota(jnp.int32, (n, n * pairs), 1)
    lane = lax.broadcasted_iota(jnp.int32, (n, LANES), 1)
    spread = jnp.broadcast_to(orders_row, (n, n * pairs)).astype(jnp.float32)

    def fill_basis(p, out, eo):
        low = jnp.sum(jnp.where(slot == source * pairs + p, spread, 0.0), axis=1, keepdims=True).astype(jnp.int32)
        even = even_order(low, degree)
        order = jnp.where(eo == 0, even, degree - even)
        order = jnp.broadcast_to(order, (n, LANES))
        factor = jnp.where(order == 0, 1.0, 2.0)
        coarse_angle = ((order * (LANES * lane)) & (NLON - 1)).astype(jnp.float32) * scale
        fine_angle = ((order * lane) & (NLON - 1)).astype(jnp.float32) * scale
        cos_coarse, sin_coarse = factor * jnp.cos(coarse_angle), factor * jnp.sin(coarse_angle)
        cos_fine, sin_fine = jnp.cos(fine_angle), jnp.sin(fine_angle)
        for tile in range(HALF // LANES):
            cc, ss = cos_coarse[:, tile : tile + 1], sin_coarse[:, tile : tile + 1]
            lanes = slice(tile * LANES, (tile + 1) * LANES)
            out[eo, :n, lanes] = (cc * cos_fine - ss * sin_fine).astype(jnp.bfloat16)
            out[eo, n:, lanes] = (-(ss * cos_fine + cc * sin_fine)).astype(jnp.bfloat16)

    @pl.loop(0, 2)
    def _(eo):
        fill_basis(0, basis_first, eo)

    @pl.loop(1, SPOTS)
    def _(j):
        far_copy(j).wait()

    partial[1] = partial[0] + jnp.sum(far[1:], axis=0)

    @pl.loop(1, COLUMN)
    def _(j):
        near_copy(j).start()

    @pl.loop(0, 2)
    def _(eo):
        fill_basis(1, basis_ref, eo)

    def finish(p, out):
        all_blocks(p).wait_recv()
        wide[...] = recv[p].astype(jnp.float32)
        for eo in range(2):
            for cycle in range(cycles):
                tile = jnp.transpose(wide[pl.ds(eo * cycles + cycle, n, stride=per_peer), :]).astype(jnp.bfloat16)
                rows = slice(cycle * fields, (cycle + 1) * fields)
                out[eo, rows, :n] = tile[:fields]
                out[eo, rows, n:] = tile[fields:]

    finish(0, held_first)

    @pl.loop(0, HALF // block)
    def _(tile):
        lanes = pl.ds(pl.multiple_of(tile * block, block), block)
        for eo in range(2):
            sum_ref[eo, :, lanes] = jnp.dot(held_first[eo], basis_first[eo, :, lanes], preferred_element_type=jnp.float32)

    finish(1, held_ref)

    @pl.loop(1, COLUMN)
    def _(j):
        near_copy(j).wait()

    total_ref[...] = partial[1] + jnp.sum(near[1:], axis=0)
    for p in range(pairs):
        all_blocks(p).wait_send()


def wave_kernel(scale, sum_ref, held_ref, basis_ref, total_ref, out_hbm, energy_ref, out, out_sem):
    cycles, fields, _ = out.shape
    width = 256
    tiles = HALF // width

    def out_copy(tile, side):
        columns = pl.ds(pl.multiple_of(side * HALF + tile * width, width), width)
        return pltpu.make_async_copy(out.at[:, :, columns], out_hbm.at[:, :, columns], out_sem.at[tile, side])

    @pl.loop(0, tiles, unroll=8)
    def _(tile):
        columns = pl.ds(pl.multiple_of(tile * width, width), width)
        even = sum_ref[0, :, columns] + jnp.dot(held_ref[0], basis_ref[0, :, columns], preferred_element_type=jnp.float32)
        odd = sum_ref[1, :, columns] + jnp.dot(held_ref[1], basis_ref[1, :, columns], preferred_element_type=jnp.float32)
        out[:, :, columns] = (even + odd).astype(jnp.bfloat16).reshape(cycles, fields, width)
        mirrored = pl.ds(pl.multiple_of(HALF + tile * width, width), width)
        out[:, :, mirrored] = (even - odd).astype(jnp.bfloat16).reshape(cycles, fields, width)
        for side in range(2):
            out_copy(tile, side).start()

    energy_ref[...] = (total_ref[:, :fields] + total_ref[:, fields:]) * scale

    @pl.loop(0, tiles)
    def _(tile):
        for side in range(2):
            out_copy(tile, side).wait()


def shards(load_coef, legendre, slab_orders, cycle_rows):
    n = lax.axis_size("blk")
    pairs, slab_rows, streams = load_coef.shape
    fields = streams // 2
    lat_count = legendre.shape[2]
    cycles = lat_count // n
    deep = (slab_rows - 1) * pairs
    per_peer = 2 * cycles
    table = jnp.transpose(legendre, (1, 0, 2))
    coef = jnp.transpose(load_coef, (1, 0, 2))
    blocks = lat_count // LANES
    anywhere = pl.BlockSpec(memory_space=pltpu.HBM)
    vmem = pl.BlockSpec(memory_space=pltpu.VMEM)
    dma = pltpu.SemaphoreType.DMA
    first, held, basis, total = pl.pallas_call(
        exchange_kernel,
        out_shape=[
            jax.ShapeDtypeStruct((2, cycles * fields, HALF), jnp.float32),
            jax.ShapeDtypeStruct((2, cycles * fields, 2 * n), jnp.bfloat16),
            jax.ShapeDtypeStruct((2, 2 * n, HALF), jnp.bfloat16),
            jax.ShapeDtypeStruct((1, streams), jnp.float32),
        ],
        in_specs=[anywhere] * 4,
        out_specs=[vmem] * 4,
        scratch_shapes=[
            pltpu.VMEM((blocks, deep, LANES), jnp.bfloat16),
            pltpu.VMEM((1, pairs, lat_count), jnp.bfloat16),
            pltpu.VMEM((deep, streams), jnp.bfloat16),
            pltpu.VMEM((1, pairs, streams), jnp.bfloat16),
            pltpu.VMEM((lat_count // LANES, LANES), jnp.int32),
            pltpu.VMEM((1, n * pairs), jnp.int32),
            pltpu.VMEM((2 * pairs * streams, deep), jnp.bfloat16),
            pltpu.VMEM((2 * pairs * streams, LANES), jnp.float32),
            pltpu.VMEM((lat_count, lat_count), jnp.bfloat16),
            pltpu.VMEM((2 * pairs * streams, lat_count), jnp.bfloat16),
            pltpu.VMEM((pairs, n * per_peer, streams), jnp.bfloat16),
            pltpu.VMEM((pairs, n * per_peer, streams), jnp.bfloat16),
            pltpu.VMEM((n * per_peer, streams), jnp.float32),
            pltpu.VMEM((2, 1, streams), jnp.float32),
            pltpu.VMEM((COLUMN, 1, streams), jnp.float32),
            pltpu.VMEM((SPOTS, 1, streams), jnp.float32),
            pltpu.VMEM((2, cycles * fields, 2 * n), jnp.bfloat16),
            pltpu.VMEM((2, 2 * n, HALF), jnp.bfloat16),
            dma((5,)),
            dma((blocks,)),
            pltpu.SemaphoreType.REGULAR,
            dma((pairs,)),
            dma((pairs,)),
            dma((COLUMN,)),
            dma((COLUMN,)),
            dma((SPOTS,)),
            dma((SPOTS,)),
        ],
        compiler_params=pltpu.CompilerParams(collective_id=0, has_side_effects=True, vmem_limit_bytes=36 * 2**20),
        name="exchange",
    )(*[pltpu.with_memory_space_constraint(x, pltpu.HBM) for x in (table, coef, cycle_rows.reshape(lat_count // LANES, LANES), slab_orders.reshape(1, n * pairs))])
    potential, mean_square = pl.pallas_call(
        functools.partial(wave_kernel, 1.0 / lat_count),
        out_shape=[
            jax.ShapeDtypeStruct((cycles, fields, NLON), jnp.bfloat16),
            jax.ShapeDtypeStruct((1, fields), jnp.float32),
        ],
        in_specs=[vmem] * 4,
        out_specs=[anywhere, vmem],
        scratch_shapes=[
            pltpu.VMEM((cycles, fields, NLON), jnp.bfloat16),
            dma((HALF // 256, 2)),
        ],
        compiler_params=pltpu.CompilerParams(vmem_limit_bytes=24 * 2**20),
        name="wave",
    )(first, held, basis, total)
    return potential, mean_square.reshape(fields)


def solution(mesh):
    in_specs = (P("blk", None, "rep"), P("blk", None, None), P(), P())
    out_specs = (P("blk", "rep", None), P("rep"))
    return jax.shard_map(shards, mesh=mesh, in_specs=in_specs, out_specs=out_specs, check_vma=False)
```

```python
import functools
import math

import jax
import jax.numpy as jnp
from jax import lax
from jax.experimental import pallas as pl
from jax.experimental.pallas import tpu as pltpu
from jax.sharding import PartitionSpec as P

NLON = 4096
HALF = NLON // 2
LANES = 128
MESH = pl.DeviceIdType.MESH
PLANES = 4
SPOTS = 16
CORES = 2
PER_PLANE = SPOTS * CORES
COLUMN = PLANES * CORES
HOPS = (2, 1, 3, 0)


def even_order(low, degree):
    return jnp.where((low & 1) == 0, low, degree - low)


def exchange_kernel(
    table_hbm, coef_hbm, rows_hbm, orders_hbm,
    sum_ref, held_ref, basis_ref, total_ref,
    table, table_last, coef, coef_last, rows_v, orders_v, masked, extra, chosen, spectra, send, recv, wide, partial, near, far, held_first, basis_first,
    in_sem, table_sem, ready_sem, send_sem, recv_sem, near_send, near_recv, far_send, far_recv,
):
    slab_rows, pairs, lat_count = table_hbm.shape
    blocks = table.shape[0]
    block = 2 * LANES
    deep = masked.shape[1]
    last = slab_rows - 1
    degree = slab_rows - 2
    streams = coef.shape[1]
    fields = streams // 2
    n = PLANES * PER_PLANE
    per_peer = 2 * (lat_count // n)
    cycles = lat_count // n
    plane_rows = PER_PLANE * per_peer

    me = lax.axis_index("blk")
    plane = me // PER_PLANE
    inside = me % PER_PLANE
    spot = inside // CORES
    core = me % CORES

    coef_copy = pltpu.make_async_copy(coef_hbm.reshape(slab_rows * pairs, streams).at[pl.ds(0, deep)], coef, in_sem.at[0])
    tail_copy = pltpu.make_async_copy(coef_hbm.at[pl.ds(last, 1)], coef_last, in_sem.at[4])
    rows_copy = pltpu.make_async_copy(rows_hbm, rows_v, in_sem.at[1])
    orders_copy = pltpu.make_async_copy(orders_hbm, orders_v, in_sem.at[2])

    last_copy = pltpu.make_async_copy(table_hbm.at[pl.ds(last, 1)], table_last, in_sem.at[3])

    def table_copy(b):
        flat = table_hbm.reshape(slab_rows * pairs, lat_count)
        return pltpu.make_async_copy(flat.at[pl.ds(0, deep), pl.ds(pl.multiple_of(b * LANES, LANES), LANES)], table.at[b], table_sem.at[b])

    rows_copy.start()
    orders_copy.start()
    last_copy.start()
    tail_copy.start()
    coef_copy.start()

    def column_peer(j):
        q = lax.rem(plane * CORES + core + j, COLUMN)
        return (q // CORES) * PER_PLANE + spot * CORES + q % CORES

    def spot_peer(j):
        return plane * PER_PLANE + lax.rem(spot + j, SPOTS) * CORES + core

    barrier = pltpu.get_barrier_semaphore()

    @pl.loop(1, COLUMN)
    def _(j):
        pl.semaphore_signal(barrier, inc=1, device_id={"blk": column_peer(j)}, device_id_type=MESH)

    for b in range(blocks):
        table_copy(b).start()

    @pl.loop(1, SPOTS)
    def _(j):
        pl.semaphore_signal(barrier, inc=1, device_id={"blk": spot_peer(j)}, device_id_type=MESH)

    rows_copy.wait()
    orders_copy.wait()
    last_copy.wait()
    tail_copy.wait()
    columns = jnp.transpose(jnp.broadcast_to(rows_v[...].astype(jnp.float32)[None], (LANES // 8, 8, LANES)).reshape(LANES, LANES))
    cycle_id = lax.broadcasted_iota(jnp.int32, (LANES, lat_count), 1).astype(jnp.float32)
    for part in range(lat_count // LANES):
        chosen[part * LANES : (part + 1) * LANES, :] = (columns[:, part : part + 1] == cycle_id).astype(jnp.float32).astype(jnp.bfloat16)
    orders_row = orders_v[...]
    slot_id = lax.broadcasted_iota(jnp.int32, orders_row.shape, 1)
    lows = [jnp.sum(jnp.where(slot_id == me * pairs + p, orders_row, 0).astype(jnp.float32), axis=1, keepdims=True).astype(jnp.int32) for p in range(pairs)]

    coef_copy.wait()
    flipped = jnp.transpose(coef[...])
    tail = coef_last[0].astype(jnp.float32)
    tail = jnp.transpose(jnp.concatenate([tail, jnp.zeros((8 - pairs, streams), jnp.float32)], axis=0))
    packed_id = lax.broadcasted_iota(jnp.int32, (1, deep), 1)
    row_id = packed_id // pairs
    pair_id = packed_id % pairs

    def mask(p):
        is_even = (lows[p] & 1) == 0
        lower = jnp.where(row_id < last - lows[p], 1, 0)
        in_even = lower == jnp.where(is_even, 1, 0)
        for eo in range(2):
            keep = jnp.where(pair_id == p, jnp.where(in_even, 1.0 - eo, 1.0 * eo), 0.0).astype(jnp.bfloat16)
            start = (2 * p + eo) * streams
            masked[start : start + streams, :] = flipped * jnp.broadcast_to(keep, flipped.shape)
            mine = jnp.where(is_even, 1.0 * eo, 1.0 - eo)
            extra[start : start + streams, :] = jnp.broadcast_to(tail[:, p : p + 1] * mine, (streams, LANES))

    mask(0)
    pl.semaphore_wait(barrier, COLUMN - 1 + SPOTS - 1)

    @pl.loop(1, SPOTS)
    def _(j):
        pl.semaphore_signal(ready_sem, inc=1, device_id={"blk": spot_peer(j)}, device_id_type=MESH)

    def spectra_of(p, first):
        rows = slice(p * 2 * streams, (p + 1) * 2 * streams)

        @pl.loop(0, lat_count // block)
        def _(b):
            if first:
                table_copy(2 * b).wait()
                table_copy(2 * b + 1).wait()
            right = jnp.concatenate([table[2 * b + i] for i in range(2)], axis=1)
            product = jnp.dot(masked[rows, :], right, preferred_element_type=jnp.float32)
            row = table_last[0, :, pl.ds(pl.multiple_of(b * block, block), block)].astype(jnp.float32)[p : p + 1, :]
            product = product + jnp.concatenate([extra[rows, :]] * (block // LANES), axis=1) * row
            spectra[rows, pl.ds(pl.multiple_of(b * block, block), block)] = product.astype(jnp.bfloat16)

    def sort_plane(p, target):
        count = PER_PLANE * cycles
        picked = chosen[pl.ds(pl.multiple_of(target * count, count), count), :]
        rows = lax.dot_general(picked, spectra[p * 2 * streams : (p + 1) * 2 * streams, :], (((1,), (1,)), ((), ())), preferred_element_type=jnp.float32)
        parts = [rows[:, eo * streams : (eo + 1) * streams].reshape(PER_PLANE, 1, cycles, streams) for eo in range(2)]
        message = jnp.concatenate(parts, axis=1).reshape(plane_rows, streams)
        send[p, pl.ds(pl.multiple_of(target * plane_rows, plane_rows), plane_rows), :] = message.astype(jnp.bfloat16)
        return jnp.sum(rows * rows, axis=0, keepdims=True)

    def block_rows(q):
        return pl.ds(pl.multiple_of(q * per_peer, per_peer), per_peer)

    def send_plane(p, hop):
        target = lax.rem(plane + hop, PLANES)

        @pl.loop(1 if hop == 0 else 0, PER_PLANE)
        def _(i):
            peer = target * PER_PLANE + lax.rem(spot + i // CORES, SPOTS) * CORES + lax.rem(core + i, CORES)
            pltpu.make_async_remote_copy(
                src_ref=send.at[p, block_rows(peer), :], dst_ref=recv.at[p, block_rows(me), :],
                send_sem=send_sem.at[p], recv_sem=recv_sem.at[p],
                device_id={"blk": peer}, device_id_type=MESH).start()

    def all_blocks(p):
        whole = pl.ds(0, (n - 1) * per_peer)
        return pltpu.make_async_remote_copy(
            src_ref=send.at[p, whole, :], dst_ref=recv.at[p, whole, :], send_sem=send_sem.at[p], recv_sem=recv_sem.at[p],
            device_id={"blk": column_peer(1)}, device_id_type=MESH)

    def keep_own(p):
        recv[p, block_rows(me), :] = send[p, block_rows(me), :]

    lane_id = lax.broadcasted_iota(jnp.int32, (1, streams), 1)

    def weighted(p, squares):
        even = even_order(lows[p], degree)
        out = jnp.zeros((1, streams), jnp.float32)
        for eo in range(2):
            order = even if eo == 0 else degree - even
            weight = jnp.where(order == 0, jnp.where(lane_id < fields, 1.0, 0.0), 2.0)
            out = out + weight * squares[:, eo * streams : (eo + 1) * streams]
        return out

    spectra_of(0, True)
    squares = sort_plane(0, lax.rem(plane + HOPS[0], PLANES))
    pl.semaphore_wait(ready_sem, SPOTS - 1)
    send_plane(0, HOPS[0])
    for hop in HOPS[1:]:
        squares = squares + sort_plane(0, lax.rem(plane + hop, PLANES))
        send_plane(0, hop)
    keep_own(0)
    energy = weighted(0, squares)
    mask(1)

    for p in range(1, pairs):
        spectra_of(p, False)
        squares = sort_plane(p, plane)
        for hop in HOPS[:-1]:
            squares = squares + sort_plane(p, lax.rem(plane + hop, PLANES))
        keep_own(p)
        energy = energy + weighted(p, squares)
    partial[0] = energy

    def near_copy(j):
        return pltpu.make_async_remote_copy(
            src_ref=partial.at[1], dst_ref=near.at[j], send_sem=near_send.at[j], recv_sem=near_recv.at[j],
            device_id={"blk": column_peer(j)}, device_id_type=MESH)

    def far_copy(j):
        return pltpu.make_async_remote_copy(
            src_ref=partial.at[0], dst_ref=far.at[j], send_sem=far_send.at[j], recv_sem=far_recv.at[j],
            device_id={"blk": spot_peer(j)}, device_id_type=MESH)

    @pl.loop(1, SPOTS)
    def _(j):
        far_copy(j).start()

    for hop in HOPS:
        send_plane(1, hop)

    scale = 2.0 * math.pi / NLON
    source = lax.broadcasted_iota(jnp.int32, (n, n * pairs), 0)
    slot = lax.broadcasted_iota(jnp.int32, (n, n * pairs), 1)
    lane = lax.broadcasted_iota(jnp.int32, (n, LANES), 1)
    spread = jnp.broadcast_to(orders_row, (n, n * pairs)).astype(jnp.float32)

    def fill_basis(p, out, eo):
        low = jnp.sum(jnp.where(slot == source * pairs + p, spread, 0.0), axis=1, keepdims=True).astype(jnp.int32)
        even = even_order(low, degree)
        order = jnp.where(eo == 0, even, degree - even)
        order = jnp.broadcast_to(order, (n, LANES))
        factor = jnp.where(order == 0, 1.0, 2.0)
        coarse_angle = ((order * (LANES * lane)) & (NLON - 1)).astype(jnp.float32) * scale
        fine_angle = ((order * lane) & (NLON - 1)).astype(jnp.float32) * scale
        cos_coarse, sin_coarse = factor * jnp.cos(coarse_angle), factor * jnp.sin(coarse_angle)
        cos_fine, sin_fine = jnp.cos(fine_angle), jnp.sin(fine_angle)
        for tile in range(HALF // LANES):
            cc, ss = cos_coarse[:, tile : tile + 1], sin_coarse[:, tile : tile + 1]
            lanes = slice(tile * LANES, (tile + 1) * LANES)
            out[eo, :n, lanes] = (cc * cos_fine - ss * sin_fine).astype(jnp.bfloat16)
            out[eo, n:, lanes] = (-(ss * cos_fine + cc * sin_fine)).astype(jnp.bfloat16)

    @pl.loop(0, 2)
    def _(eo):
        fill_basis(0, basis_first, eo)

    @pl.loop(1, SPOTS)
    def _(j):
        far_copy(j).wait()

    partial[1] = partial[0] + jnp.sum(far[1:], axis=0)

    @pl.loop(1, COLUMN)
    def _(j):
        near_copy(j).start()

    @pl.loop(0, 2)
    def _(eo):
        fill_basis(1, basis_ref, eo)

    def finish(p, out):
        all_blocks(p).wait_recv()
        arrived = recv[p].astype(jnp.float32).reshape(n, 2, cycles, streams)
        for eo in range(2):
            wide[eo] = arrived[:, eo].reshape(n * cycles, streams)
        for eo in range(2):
            for cycle in range(cycles):
                tile = jnp.transpose(wide[eo, pl.ds(cycle, n, stride=cycles), :]).astype(jnp.bfloat16)
                rows = slice(cycle * fields, (cycle + 1) * fields)
                out[eo, rows, :n] = tile[:fields]
                out[eo, rows, n:] = tile[fields:]

    finish(0, held_first)

    @pl.loop(0, HALF // block)
    def _(tile):
        lanes = pl.ds(pl.multiple_of(tile * block, block), block)
        for eo in range(2):
            sum_ref[eo, :, lanes] = jnp.dot(held_first[eo], basis_first[eo, :, lanes], preferred_element_type=jnp.float32)

    finish(1, held_ref)

    @pl.loop(1, COLUMN)
    def _(j):
        near_copy(j).wait()

    total_ref[...] = partial[1] + jnp.sum(near[1:], axis=0)
    for p in range(pairs):
        all_blocks(p).wait_send()


def wave_kernel(scale, sum_ref, held_ref, basis_ref, total_ref, out_hbm, energy_hbm, out, energy, out_sem, energy_sem):
    cycles, fields, _ = out.shape
    width = 256
    tiles = HALF // width

    def out_copy(tile, side):
        columns = pl.ds(pl.multiple_of(side * HALF + tile * width, width), width)
        return pltpu.make_async_copy(out.at[:, :, columns], out_hbm.at[:, :, columns], out_sem.at[tile, side])

    energy[...] = (total_ref[:, :fields] + total_ref[:, fields:]) * scale
    energy_copy = pltpu.make_async_copy(energy, energy_hbm, energy_sem)

    @pl.loop(0, tiles, unroll=8)
    def _(tile):
        columns = pl.ds(pl.multiple_of(tile * width, width), width)
        even = sum_ref[0, :, columns] + jnp.dot(held_ref[0], basis_ref[0, :, columns], preferred_element_type=jnp.float32)
        odd = sum_ref[1, :, columns] + jnp.dot(held_ref[1], basis_ref[1, :, columns], preferred_element_type=jnp.float32)
        out[:, :, columns] = (even + odd).astype(jnp.bfloat16).reshape(cycles, fields, width)
        mirrored = pl.ds(pl.multiple_of(HALF + tile * width, width), width)
        out[:, :, mirrored] = (even - odd).astype(jnp.bfloat16).reshape(cycles, fields, width)
        for side in range(2):
            out_copy(tile, side).start()

    energy_copy.start()

    @pl.loop(0, tiles)
    def _(tile):
        for side in range(2):
            out_copy(tile, side).wait()

    energy_copy.wait()


def shards(load_coef, legendre, slab_orders, cycle_rows):
    n = lax.axis_size("blk")
    pairs, slab_rows, streams = load_coef.shape
    fields = streams // 2
    lat_count = legendre.shape[2]
    cycles = lat_count // n
    deep = (slab_rows - 1) * pairs
    per_peer = 2 * cycles
    table = jnp.transpose(legendre, (1, 0, 2))
    coef = jnp.transpose(load_coef, (1, 0, 2))
    blocks = lat_count // LANES
    anywhere = pl.BlockSpec(memory_space=pltpu.HBM)
    vmem = pl.BlockSpec(memory_space=pltpu.VMEM)
    dma = pltpu.SemaphoreType.DMA
    first, held, basis, total = pl.pallas_call(
        exchange_kernel,
        out_shape=[
            jax.ShapeDtypeStruct((2, cycles * fields, HALF), jnp.float32),
            jax.ShapeDtypeStruct((2, cycles * fields, 2 * n), jnp.bfloat16),
            jax.ShapeDtypeStruct((2, 2 * n, HALF), jnp.bfloat16),
            jax.ShapeDtypeStruct((1, streams), jnp.float32),
        ],
        in_specs=[anywhere] * 4,
        out_specs=[vmem] * 4,
        scratch_shapes=[
            pltpu.VMEM((blocks, deep, LANES), jnp.bfloat16),
            pltpu.VMEM((1, pairs, lat_count), jnp.bfloat16),
            pltpu.VMEM((deep, streams), jnp.bfloat16),
            pltpu.VMEM((1, pairs, streams), jnp.bfloat16),
            pltpu.VMEM((lat_count // LANES, LANES), jnp.int32),
            pltpu.VMEM((1, n * pairs), jnp.int32),
            pltpu.VMEM((2 * pairs * streams, deep), jnp.bfloat16),
            pltpu.VMEM((2 * pairs * streams, LANES), jnp.float32),
            pltpu.VMEM((lat_count, lat_count), jnp.bfloat16),
            pltpu.VMEM((2 * pairs * streams, lat_count), jnp.bfloat16),
            pltpu.VMEM((pairs, n * per_peer, streams), jnp.bfloat16),
            pltpu.VMEM((pairs, n * per_peer, streams), jnp.bfloat16),
            pltpu.VMEM((2, n * cycles, streams), jnp.float32),
            pltpu.VMEM((2, 1, streams), jnp.float32),
            pltpu.VMEM((COLUMN, 1, streams), jnp.float32),
            pltpu.VMEM((SPOTS, 1, streams), jnp.float32),
            pltpu.VMEM((2, cycles * fields, 2 * n), jnp.bfloat16),
            pltpu.VMEM((2, 2 * n, HALF), jnp.bfloat16),
            dma((5,)),
            dma((blocks,)),
            pltpu.SemaphoreType.REGULAR,
            dma((pairs,)),
            dma((pairs,)),
            dma((COLUMN,)),
            dma((COLUMN,)),
            dma((SPOTS,)),
            dma((SPOTS,)),
        ],
        compiler_params=pltpu.CompilerParams(collective_id=0, has_side_effects=True, vmem_limit_bytes=36 * 2**20),
        name="exchange",
    )(*[pltpu.with_memory_space_constraint(x, pltpu.HBM) for x in (table, coef, cycle_rows.reshape(lat_count // LANES, LANES), slab_orders.reshape(1, n * pairs))])
    potential, mean_square = pl.pallas_call(
        functools.partial(wave_kernel, 1.0 / lat_count),
        out_shape=[
            jax.ShapeDtypeStruct((cycles, fields, NLON), jnp.bfloat16),
            jax.ShapeDtypeStruct((1, fields), jnp.float32),
        ],
        in_specs=[vmem] * 4,
        out_specs=[anywhere, anywhere],
        scratch_shapes=[
            pltpu.VMEM((cycles, fields, NLON), jnp.bfloat16),
            pltpu.VMEM((1, fields), jnp.float32),
            dma((HALF // 256, 2)),
            dma,
        ],
        compiler_params=pltpu.CompilerParams(vmem_limit_bytes=24 * 2**20),
        name="wave",
    )(first, held, basis, total)
    return potential, mean_square.reshape(fields)


def solution(mesh):
    in_specs = (P("blk", None, "rep"), P("blk", None, None), P(), P())
    out_specs = (P("blk", "rep", None), P("rep"))
    return jax.shard_map(shards, mesh=mesh, in_specs=in_specs, out_specs=out_specs, check_vma=False)
```

```python
import functools
import math

import jax
import jax.numpy as jnp
from jax import lax
from jax.experimental import pallas as pl
from jax.experimental.pallas import tpu as pltpu
from jax.sharding import PartitionSpec as P

NLON = 4096
HALF = NLON // 2
LANES = 128
MESH = pl.DeviceIdType.MESH
PLANES = 4
SPOTS = 16
CORES = 2
PER_PLANE = SPOTS * CORES
COLUMN = PLANES * CORES
HOPS = (2, 1, 3, 0)
FINAL_HOPS = ((2, 1, 0, 3), (2, 0, 3, 1), (2, 3, 0, 1), (1, 2, 0, 3))


def even_order(low, degree):
    return jnp.where((low & 1) == 0, low, degree - low)


def exchange_kernel(
    table_hbm, coef_hbm, rows_hbm, orders_hbm,
    sum_ref, held_ref, basis_ref, total_ref,
    table, table_last, coef, coef_last, rows_v, orders_v, masked, extra, chosen, spectra, send, recv, wide, partial, near, far, held_first, basis_first,
    in_sem, table_sem, ready_sem, send_sem, recv_sem, near_send, near_recv, far_send, far_recv,
):
    slab_rows, pairs, lat_count = table_hbm.shape
    blocks = table.shape[0]
    block = 2 * LANES
    deep = masked.shape[1]
    last = slab_rows - 1
    degree = slab_rows - 2
    streams = coef.shape[1]
    fields = streams // 2
    n = PLANES * PER_PLANE
    per_peer = 2 * (lat_count // n)
    cycles = lat_count // n
    plane_rows = PER_PLANE * per_peer

    me = lax.axis_index("blk")
    plane = me // PER_PLANE
    inside = me % PER_PLANE
    spot = inside // CORES
    core = me % CORES

    coef_copy = pltpu.make_async_copy(coef_hbm.reshape(slab_rows * pairs, streams).at[pl.ds(0, deep)], coef, in_sem.at[0])
    tail_copy = pltpu.make_async_copy(coef_hbm.at[pl.ds(last, 1)], coef_last, in_sem.at[4])
    rows_copy = pltpu.make_async_copy(rows_hbm, rows_v, in_sem.at[1])
    orders_copy = pltpu.make_async_copy(orders_hbm, orders_v, in_sem.at[2])

    last_copy = pltpu.make_async_copy(table_hbm.at[pl.ds(last, 1)], table_last, in_sem.at[3])

    def table_copy(b):
        flat = table_hbm.reshape(slab_rows * pairs, lat_count)
        return pltpu.make_async_copy(flat.at[pl.ds(0, deep), pl.ds(pl.multiple_of(b * LANES, LANES), LANES)], table.at[b], table_sem.at[b])

    rows_copy.start()
    orders_copy.start()
    last_copy.start()
    tail_copy.start()
    coef_copy.start()

    def column_peer(j):
        q = lax.rem(plane * CORES + core + j, COLUMN)
        return (q // CORES) * PER_PLANE + spot * CORES + q % CORES

    def spot_peer(j):
        return plane * PER_PLANE + lax.rem(spot + j, SPOTS) * CORES + core

    barrier = pltpu.get_barrier_semaphore()

    @pl.loop(1, COLUMN)
    def _(j):
        pl.semaphore_signal(barrier, inc=1, device_id={"blk": column_peer(j)}, device_id_type=MESH)

    for b in range(blocks):
        table_copy(b).start()

    @pl.loop(1, SPOTS)
    def _(j):
        pl.semaphore_signal(barrier, inc=1, device_id={"blk": spot_peer(j)}, device_id_type=MESH)

    rows_copy.wait()
    orders_copy.wait()
    last_copy.wait()
    tail_copy.wait()
    columns = jnp.transpose(jnp.broadcast_to(rows_v[...].astype(jnp.float32)[None], (LANES // 8, 8, LANES)).reshape(LANES, LANES))
    cycle_id = lax.broadcasted_iota(jnp.int32, (LANES, lat_count), 1).astype(jnp.float32)
    for part in range(lat_count // LANES):
        chosen[part * LANES : (part + 1) * LANES, :] = (columns[:, part : part + 1] == cycle_id).astype(jnp.float32).astype(jnp.bfloat16)
    orders_row = orders_v[...]
    slot_id = lax.broadcasted_iota(jnp.int32, orders_row.shape, 1)
    lows = [jnp.sum(jnp.where(slot_id == me * pairs + p, orders_row, 0).astype(jnp.float32), axis=1, keepdims=True).astype(jnp.int32) for p in range(pairs)]

    coef_copy.wait()
    flipped = jnp.transpose(coef[...])
    tail = coef_last[0].astype(jnp.float32)
    tail = jnp.transpose(jnp.concatenate([tail, jnp.zeros((8 - pairs, streams), jnp.float32)], axis=0))
    packed_id = lax.broadcasted_iota(jnp.int32, (1, deep), 1)
    row_id = packed_id // pairs
    pair_id = packed_id % pairs

    def mask(p):
        is_even = (lows[p] & 1) == 0
        lower = jnp.where(row_id < last - lows[p], 1, 0)
        in_even = lower == jnp.where(is_even, 1, 0)
        for eo in range(2):
            keep = jnp.where(pair_id == p, jnp.where(in_even, 1.0 - eo, 1.0 * eo), 0.0).astype(jnp.bfloat16)
            start = (2 * p + eo) * streams
            masked[start : start + streams, :] = flipped * jnp.broadcast_to(keep, flipped.shape)
            mine = jnp.where(is_even, 1.0 * eo, 1.0 - eo)
            extra[start : start + streams, :] = jnp.broadcast_to(tail[:, p : p + 1] * mine, (streams, LANES))

    mask(0)
    pl.semaphore_wait(barrier, COLUMN - 1 + SPOTS - 1)

    @pl.loop(1, SPOTS)
    def _(j):
        pl.semaphore_signal(ready_sem, inc=1, device_id={"blk": spot_peer(j)}, device_id_type=MESH)

    def spectra_of(p, first):
        rows = slice(p * 2 * streams, (p + 1) * 2 * streams)

        @pl.loop(0, lat_count // block)
        def _(b):
            if first:
                table_copy(2 * b).wait()
                table_copy(2 * b + 1).wait()
            right = jnp.concatenate([table[2 * b + i] for i in range(2)], axis=1)
            product = jnp.dot(masked[rows, :], right, preferred_element_type=jnp.float32)
            row = table_last[0, :, pl.ds(pl.multiple_of(b * block, block), block)].astype(jnp.float32)[p : p + 1, :]
            product = product + jnp.concatenate([extra[rows, :]] * (block // LANES), axis=1) * row
            spectra[rows, pl.ds(pl.multiple_of(b * block, block), block)] = product.astype(jnp.bfloat16)

    def sort_plane(p, target):
        count = PER_PLANE * cycles
        picked = chosen[pl.ds(pl.multiple_of(target * count, count), count), :]
        rows = lax.dot_general(picked, spectra[p * 2 * streams : (p + 1) * 2 * streams, :], (((1,), (1,)), ((), ())), preferred_element_type=jnp.float32)
        parts = [rows[:, eo * streams : (eo + 1) * streams].reshape(PER_PLANE, 1, cycles, streams) for eo in range(2)]
        message = jnp.concatenate(parts, axis=1).reshape(plane_rows, streams)
        send[p, pl.ds(pl.multiple_of(target * plane_rows, plane_rows), plane_rows), :] = message.astype(jnp.bfloat16)
        return jnp.sum(rows * rows, axis=0, keepdims=True)

    def block_rows(q):
        return pl.ds(pl.multiple_of(q * per_peer, per_peer), per_peer)

    def send_plane(p, hop):
        target = lax.rem(plane + hop, PLANES)
        first = (1 if hop == 0 else 0) if isinstance(hop, int) else jnp.where(hop == 0, 1, 0)

        def send_one(i, carry):
            peer = target * PER_PLANE + lax.rem(spot + i // CORES, SPOTS) * CORES + lax.rem(core + i, CORES)
            pltpu.make_async_remote_copy(
                src_ref=send.at[p, block_rows(peer), :], dst_ref=recv.at[p, block_rows(me), :],
                send_sem=send_sem.at[p], recv_sem=recv_sem.at[p],
                device_id={"blk": peer}, device_id_type=MESH).start()
            return carry

        lax.fori_loop(first, PER_PLANE, send_one, 0)

    def all_blocks(p):
        whole = pl.ds(0, (n - 1) * per_peer)
        return pltpu.make_async_remote_copy(
            src_ref=send.at[p, whole, :], dst_ref=recv.at[p, whole, :], send_sem=send_sem.at[p], recv_sem=recv_sem.at[p],
            device_id={"blk": column_peer(1)}, device_id_type=MESH)

    def keep_own(p):
        recv[p, block_rows(me), :] = send[p, block_rows(me), :]

    lane_id = lax.broadcasted_iota(jnp.int32, (1, streams), 1)

    def weighted(p, squares):
        even = even_order(lows[p], degree)
        out = jnp.zeros((1, streams), jnp.float32)
        for eo in range(2):
            order = even if eo == 0 else degree - even
            weight = jnp.where(order == 0, jnp.where(lane_id < fields, 1.0, 0.0), 2.0)
            out = out + weight * squares[:, eo * streams : (eo + 1) * streams]
        return out

    spectra_of(0, True)
    squares = sort_plane(0, lax.rem(plane + HOPS[0], PLANES))
    pl.semaphore_wait(ready_sem, SPOTS - 1)
    send_plane(0, HOPS[0])
    for hop in HOPS[1:]:
        squares = squares + sort_plane(0, lax.rem(plane + hop, PLANES))
        send_plane(0, hop)
    keep_own(0)
    energy = weighted(0, squares)
    mask(1)

    for p in range(1, pairs):
        spectra_of(p, False)
        squares = sort_plane(p, plane)
        for hop in HOPS[:-1]:
            squares = squares + sort_plane(p, lax.rem(plane + hop, PLANES))
        keep_own(p)
        energy = energy + weighted(p, squares)
    partial[0] = energy

    def near_copy(j):
        return pltpu.make_async_remote_copy(
            src_ref=partial.at[1], dst_ref=near.at[j], send_sem=near_send.at[j], recv_sem=near_recv.at[j],
            device_id={"blk": column_peer(j)}, device_id_type=MESH)

    def far_copy(j):
        return pltpu.make_async_remote_copy(
            src_ref=partial.at[0], dst_ref=far.at[j], send_sem=far_send.at[j], recv_sem=far_recv.at[j],
            device_id={"blk": spot_peer(j)}, device_id_type=MESH)

    @pl.loop(1, SPOTS)
    def _(j):
        far_copy(j).start()

    for step in range(PLANES):
        send_plane(1, sum(jnp.where(plane == z, FINAL_HOPS[z][step], 0) for z in range(PLANES)))

    scale = 2.0 * math.pi / NLON
    source = lax.broadcasted_iota(jnp.int32, (n, n * pairs), 0)
    slot = lax.broadcasted_iota(jnp.int32, (n, n * pairs), 1)
    lane = lax.broadcasted_iota(jnp.int32, (n, LANES), 1)
    spread = jnp.broadcast_to(orders_row, (n, n * pairs)).astype(jnp.float32)

    def fill_basis(p, out, eo):
        low = jnp.sum(jnp.where(slot == source * pairs + p, spread, 0.0), axis=1, keepdims=True).astype(jnp.int32)
        even = even_order(low, degree)
        order = jnp.where(eo == 0, even, degree - even)
        order = jnp.broadcast_to(order, (n, LANES))
        factor = jnp.where(order == 0, 1.0, 2.0)
        coarse_angle = ((order * (LANES * lane)) & (NLON - 1)).astype(jnp.float32) * scale
        fine_angle = ((order * lane) & (NLON - 1)).astype(jnp.float32) * scale
        cos_coarse, sin_coarse = factor * jnp.cos(coarse_angle), factor * jnp.sin(coarse_angle)
        cos_fine, sin_fine = jnp.cos(fine_angle), jnp.sin(fine_angle)
        for tile in range(HALF // LANES):
            cc, ss = cos_coarse[:, tile : tile + 1], sin_coarse[:, tile : tile + 1]
            lanes = slice(tile * LANES, (tile + 1) * LANES)
            out[eo, :n, lanes] = (cc * cos_fine - ss * sin_fine).astype(jnp.bfloat16)
            out[eo, n:, lanes] = (-(ss * cos_fine + cc * sin_fine)).astype(jnp.bfloat16)

    @pl.loop(0, 2)
    def _(eo):
        fill_basis(0, basis_first, eo)

    @pl.loop(1, SPOTS)
    def _(j):
        far_copy(j).wait()

    partial[1] = partial[0] + jnp.sum(far[1:], axis=0)

    @pl.loop(1, COLUMN)
    def _(j):
        near_copy(j).start()

    @pl.loop(0, 2)
    def _(eo):
        fill_basis(1, basis_ref, eo)

    def finish(p, out):
        all_blocks(p).wait_recv()
        arrived = recv[p].astype(jnp.float32).reshape(n, 2, cycles, streams)
        for eo in range(2):
            wide[eo] = arrived[:, eo].reshape(n * cycles, streams)
        for eo in range(2):
            for cycle in range(cycles):
                tile = jnp.transpose(wide[eo, pl.ds(cycle, n, stride=cycles), :]).astype(jnp.bfloat16)
                rows = slice(cycle * fields, (cycle + 1) * fields)
                out[eo, rows, :n] = tile[:fields]
                out[eo, rows, n:] = tile[fields:]

    finish(0, held_first)

    @pl.loop(0, HALF // block)
    def _(tile):
        lanes = pl.ds(pl.multiple_of(tile * block, block), block)
        for eo in range(2):
            sum_ref[eo, :, lanes] = jnp.dot(held_first[eo], basis_first[eo, :, lanes], preferred_element_type=jnp.float32)

    finish(1, held_ref)

    @pl.loop(1, COLUMN)
    def _(j):
        near_copy(j).wait()

    total_ref[...] = partial[1] + jnp.sum(near[1:], axis=0)
    for p in range(pairs):
        all_blocks(p).wait_send()


def wave_kernel(scale, sum_ref, held_ref, basis_ref, total_ref, out_hbm, energy_hbm, out, energy, out_sem, energy_sem):
    cycles, fields, _ = out.shape
    width = 256
    tiles = HALF // width

    def out_copy(tile, side):
        columns = pl.ds(pl.multiple_of(side * HALF + tile * width, width), width)
        return pltpu.make_async_copy(out.at[:, :, columns], out_hbm.at[:, :, columns], out_sem.at[tile, side])

    energy[...] = (total_ref[:, :fields] + total_ref[:, fields:]) * scale
    energy_copy = pltpu.make_async_copy(energy, energy_hbm, energy_sem)

    @pl.loop(0, tiles, unroll=8)
    def _(tile):
        columns = pl.ds(pl.multiple_of(tile * width, width), width)
        even = sum_ref[0, :, columns] + jnp.dot(held_ref[0], basis_ref[0, :, columns], preferred_element_type=jnp.float32)
        odd = sum_ref[1, :, columns] + jnp.dot(held_ref[1], basis_ref[1, :, columns], preferred_element_type=jnp.float32)
        out[:, :, columns] = (even + odd).astype(jnp.bfloat16).reshape(cycles, fields, width)
        mirrored = pl.ds(pl.multiple_of(HALF + tile * width, width), width)
        out[:, :, mirrored] = (even - odd).astype(jnp.bfloat16).reshape(cycles, fields, width)
        for side in range(2):
            out_copy(tile, side).start()

    energy_copy.start()

    @pl.loop(0, tiles)
    def _(tile):
        for side in range(2):
            out_copy(tile, side).wait()

    energy_copy.wait()


def shards(load_coef, legendre, slab_orders, cycle_rows):
    n = lax.axis_size("blk")
    pairs, slab_rows, streams = load_coef.shape
    fields = streams // 2
    lat_count = legendre.shape[2]
    cycles = lat_count // n
    deep = (slab_rows - 1) * pairs
    per_peer = 2 * cycles
    table = jnp.transpose(legendre, (1, 0, 2))
    coef = jnp.transpose(load_coef, (1, 0, 2))
    blocks = lat_count // LANES
    anywhere = pl.BlockSpec(memory_space=pltpu.HBM)
    vmem = pl.BlockSpec(memory_space=pltpu.VMEM)
    dma = pltpu.SemaphoreType.DMA
    first, held, basis, total = pl.pallas_call(
        exchange_kernel,
        out_shape=[
            jax.ShapeDtypeStruct((2, cycles * fields, HALF), jnp.float32),
            jax.ShapeDtypeStruct((2, cycles * fields, 2 * n), jnp.bfloat16),
            jax.ShapeDtypeStruct((2, 2 * n, HALF), jnp.bfloat16),
            jax.ShapeDtypeStruct((1, streams), jnp.float32),
        ],
        in_specs=[anywhere] * 4,
        out_specs=[vmem] * 4,
        scratch_shapes=[
            pltpu.VMEM((blocks, deep, LANES), jnp.bfloat16),
            pltpu.VMEM((1, pairs, lat_count), jnp.bfloat16),
            pltpu.VMEM((deep, streams), jnp.bfloat16),
            pltpu.VMEM((1, pairs, streams), jnp.bfloat16),
            pltpu.VMEM((lat_count // LANES, LANES), jnp.int32),
            pltpu.VMEM((1, n * pairs), jnp.int32),
            pltpu.VMEM((2 * pairs * streams, deep), jnp.bfloat16),
            pltpu.VMEM((2 * pairs * streams, LANES), jnp.float32),
            pltpu.VMEM((lat_count, lat_count), jnp.bfloat16),
            pltpu.VMEM((2 * pairs * streams, lat_count), jnp.bfloat16),
            pltpu.VMEM((pairs, n * per_peer, streams), jnp.bfloat16),
            pltpu.VMEM((pairs, n * per_peer, streams), jnp.bfloat16),
            pltpu.VMEM((2, n * cycles, streams), jnp.float32),
            pltpu.VMEM((2, 1, streams), jnp.float32),
            pltpu.VMEM((COLUMN, 1, streams), jnp.float32),
            pltpu.VMEM((SPOTS, 1, streams), jnp.float32),
            pltpu.VMEM((2, cycles * fields, 2 * n), jnp.bfloat16),
            pltpu.VMEM((2, 2 * n, HALF), jnp.bfloat16),
            dma((5,)),
            dma((blocks,)),
            pltpu.SemaphoreType.REGULAR,
            dma((pairs,)),
            dma((pairs,)),
            dma((COLUMN,)),
            dma((COLUMN,)),
            dma((SPOTS,)),
            dma((SPOTS,)),
        ],
        compiler_params=pltpu.CompilerParams(collective_id=0, has_side_effects=True, vmem_limit_bytes=36 * 2**20),
        name="exchange",
    )(*[pltpu.with_memory_space_constraint(x, pltpu.HBM) for x in (table, coef, cycle_rows.reshape(lat_count // LANES, LANES), slab_orders.reshape(1, n * pairs))])
    potential, mean_square = pl.pallas_call(
        functools.partial(wave_kernel, 1.0 / lat_count),
        out_shape=[
            jax.ShapeDtypeStruct((cycles, fields, NLON), jnp.bfloat16),
            jax.ShapeDtypeStruct((1, fields), jnp.float32),
        ],
        in_specs=[vmem] * 4,
        out_specs=[anywhere, anywhere],
        scratch_shapes=[
            pltpu.VMEM((cycles, fields, NLON), jnp.bfloat16),
            pltpu.VMEM((1, fields), jnp.float32),
            dma((HALF // 256, 2)),
            dma,
        ],
        compiler_params=pltpu.CompilerParams(vmem_limit_bytes=24 * 2**20),
        name="wave",
    )(first, held, basis, total)
    return potential, mean_square.reshape(fields)


def solution(mesh):
    in_specs = (P("blk", None, "rep"), P("blk", None, None), P(), P())
    out_specs = (P("blk", "rep", None), P("rep"))
    return jax.shard_map(shards, mesh=mesh, in_specs=in_specs, out_specs=out_specs, check_vma=False)
```
